32 devices in a mesh: rows: 8 (over y, x, core), rhs: 4 (over z).
Axes of the slice: x: 2, y: 2, z: 4, core: 2. Of those that a mesh axis runs over, the one named last changes fastest.
Arguments:
- sources: bfloat16 [32768, 2048], P('rows', 'rhs'), may hold values from -6 to 6
- near_blocks: bfloat16 [128, 3, 256, 256], P('rows'), may hold values from -0.21875 to 0.21875
- near_list: int32 [128, 3], P('rows'), may hold values from 0 to 127, as said below
- source_basis: bfloat16 [128, 256, 32], P('rows'), may hold values from -0.375 to 0.375
- target_basis: bfloat16 [128, 256, 32], P('rows'), may hold values from -0.375 to 0.375
- transfer_fine: bfloat16 [224, 32, 32], P('rows'), may hold values from -0.875 to 0.875
- transfer_coarse: bfloat16 [32, 32, 32], P('rhs'), may hold values from -0.875 to 0.875
- couple_fine: bfloat16 [224, 3, 32, 32], P('rows'), may hold values from -0.625 to 0.625
- couple_coarse: bfloat16 [32, 3, 32, 32], P('rhs'), may hold values from -0.625 to 0.625
- far_fine: int32 [224, 3], P('rows'), may hold values from 0 to 127, as said below
- far_coarse: int32 [32, 3], replicated, may hold values from -1 to 15, as said below
Outputs:
- potentials: bfloat16 [32768, 2048], P('rows', 'rhs')
The draws below stay inside these ranges and needn't reach their ends.
Inputs may be any that keep to these rules, and one draw needn't show every extreme that they name: `near_list`: row t lists the leaf clusters t - 1, t and t + 1 modulo 128 in some order. `far_fine`: row d * 28 + o + i belongs to cluster d * m + i of the level with n = m * 8 clusters, where (o, m) is (0, 16), (16, 8) or (24, 4). It lists, in some order, the three clusters of that level that are children of the cyclic neighbours of the cluster's parent and not cyclic neighbours of the cluster: for cluster j with parent p = j // 2, the clusters 2p - 2, 2p + 2, 2p + 3 if j is even and 2p - 2, 2p - 1, 2p + 3 if j is odd, modulo n. `far_coarse`: row n + j for n = 8, 16, ..., 16 lists, in some order, the three far clusters of cluster j of the level with n clusters by the rule of far_fine. Row 4 + j holds (j + 2) modulo 4 in slot 0 and -1 in slots 1 and 2. Rows 0 to 3 hold -1.
All inputs are finite; a program needn't handle non-finite values.
Results may differ from the reference program's by a relative error of at most 0.012.
Values may be sent and summed in bfloat16 or wider, within the bound.
A program may use at most 128 MiB of HBM per device.

```python
import jax
import jax.numpy as jnp
from jax import lax

LEAF = 256
RANK = 32
LPD = 16
LEAVES = 128
POINTS = 32768
RHS = 2048
FINE = 224
COARSE = 32


def shuffle_rows(key, table):
    keys = jax.random.split(key, table.shape[0])

    def one_order(single):
        return jax.random.permutation(single, 3)
    orders = jax.vmap(one_order)(keys)
    return jnp.take_along_axis(table, orders, axis=1)


def far_rule(index, clusters):
    parent = index // 2
    second = jnp.where(index % 2 == 1, 2 * parent - 1, 2 * parent + 2)
    first = (2 * parent - 2 + 4 * clusters) % clusters
    second = (second + 4 * clusters) % clusters
    third = (2 * parent + 3) % clusters
    return jnp.stack([first, second, third], axis=1).astype(jnp.int32)


def draw_near_list(key, part):
    leaves = jnp.arange(LEAVES, dtype=jnp.int32)
    table = jnp.stack([(leaves + LEAVES - 1) % LEAVES, leaves, (leaves + 1) % LEAVES], axis=1)
    return shuffle_rows(jax.random.fold_in(key, 11), table)


def draw_far_fine(key, part):
    row_count = LEAVES // LPD
    block = LPD + LPD // 2 + LPD // 4
    rows_all = jnp.arange(row_count * block, dtype=jnp.int32)
    device = rows_all // block
    within = rows_all % block
    local_count = jnp.where(within < LPD, LPD, jnp.where(within < LPD + LPD // 2, LPD // 2, LPD // 4))
    offset = jnp.where(within < LPD, 0, jnp.where(within < LPD + LPD // 2, LPD, LPD + LPD // 2))
    index = device * local_count + within - offset
    table = far_rule(index, local_count * row_count)
    return shuffle_rows(jax.random.fold_in(key, 23), table)


def draw_far_coarse(key, part):
    row_count = LEAVES // LPD
    empty = jnp.full((4,), -1, jnp.int32)
    top = jnp.arange(4, dtype=jnp.int32)
    pieces = [jnp.full((4, 3), -1, jnp.int32), jnp.stack([(top + 2) % 4, empty, empty], axis=1)]
    clusters = 8
    for level in range((2 * row_count).bit_length() - 3):
        index = jnp.arange(clusters, dtype=jnp.int32)
        pieces.append(shuffle_rows(jax.random.fold_in(key, 100 + clusters), far_rule(index, clusters)))
        clusters = clusters * 2
    return jnp.concatenate(pieces, axis=0)


def block_scale(own_key, dims, cuts, low, largest):
    def one(position, parts):
        heights = jax.random.uniform(jax.random.fold_in(jax.random.fold_in(own_key, 6), position), (parts,), jnp.float32, low / len(cuts), largest / len(cuts))
        return jnp.repeat(jnp.exp(heights), dims[position] // parts).reshape((-1,) + (1,) * (len(dims) - position - 1))

    gain = one(*cuts[0])
    for cut in cuts[1:]:
        gain = gain * one(*cut)
    return gain


def centred(stream_key, extent, deviation, most, shards=(), held_as=jnp.bfloat16):
    gain = block_scale(stream_key, extent, shards, -0.22, 0.18) if shards else 1.0
    values = jax.random.normal(stream_key, extent, jnp.float32) * deviation * gain
    return jnp.minimum(jnp.maximum(values, -most), most).astype(held_as)


def setup_inputs(seed: int = 0) -> dict:
    splits = jax.random.split(jax.random.key(seed), 12)
    sources = centred(splits[0], (POINTS, RHS), 1.0, 6.0, ((0, 8), (1, 4)))
    near_blocks = centred(splits[1], (LEAVES, 3, LEAF, LEAF), (3 * LEAF) ** -0.5, 0.21875, ((0, 8),))
    near_list = draw_near_list(jax.random.fold_in(splits[11], 71), 0)
    source_basis = centred(splits[3], (LEAVES, LEAF, RANK), LEAF ** -0.5, 0.375, ((0, 8),))
    target_basis = centred(splits[4], (LEAVES, LEAF, RANK), (8 * RANK) ** -0.5, 0.375, ((0, 8),))
    transfer_fine = centred(splits[5], (FINE, RANK, RANK), (3 * RANK // 2) ** -0.5, 0.875, ((0, 8),))
    transfer_coarse = centred(splits[6], (COARSE, RANK, RANK), (3 * RANK // 2) ** -0.5, 0.875, ((0, 4),))
    couple_fine = centred(splits[7], (FINE, 3, RANK, RANK), (3 * RANK) ** -0.5, 0.625, ((0, 8),))
    couple_coarse = centred(splits[8], (COARSE, 3, RANK, RANK), (3 * RANK) ** -0.5, 0.625, ((0, 4),))
    far_fine = draw_far_fine(jax.random.fold_in(splits[11], 71), 0)
    far_coarse = draw_far_coarse(jax.random.fold_in(splits[11], 71), 0)
    return dict(sources=sources, near_blocks=near_blocks, near_list=near_list, source_basis=source_basis, target_basis=target_basis, transfer_fine=transfer_fine, transfer_coarse=transfer_coarse, couple_fine=couple_fine, couple_coarse=couple_coarse, far_fine=far_fine, far_coarse=far_coarse)


def fine_level(table, row_count, first, count):
    block = table.shape[0] // row_count
    shaped = table.reshape((row_count, block) + table.shape[1:])
    return shaped[:, first:first + count].reshape((row_count * count,) + table.shape[1:])


def couple(moments, blocks, partners):
    valid = partners >= 0
    picked = moments[jnp.maximum(partners, 0)]
    picked = jnp.where(valid[:, :, None, None], picked, jnp.zeros_like(picked))
    return jnp.einsum('nsab,nsbr->nar', blocks.astype(jnp.float32), picked.astype(jnp.float32))


def lift(moments, transfer):
    clusters, rank, width = moments.shape
    product = jnp.einsum('nab,nar->nbr', transfer.astype(jnp.float32), moments.astype(jnp.float32))
    return product.reshape(clusters // 2, 2, rank, width).sum(axis=1).astype(jnp.bfloat16)


def lower(parent, transfer, coupled):
    spread = jnp.repeat(parent, 2, axis=0)
    carried = jnp.einsum('nab,nbr->nar', transfer.astype(jnp.float32), spread.astype(jnp.float32))
    return (coupled + carried).astype(jnp.bfloat16)


def reference(sources, near_blocks, near_list, source_basis, target_basis, transfer_fine, transfer_coarse, couple_fine, couple_coarse, far_fine, far_coarse):
    row_count = LEAVES // LPD
    width = sources.shape[1]
    counts = [LPD, LPD // 2, LPD // 4]
    firsts = [0, LPD, LPD + LPD // 2]
    shaped = sources.reshape(LEAVES, LEAF, width)

    def leaf_moments(index):
        return jnp.dot(source_basis[index].T, shaped[index], preferred_element_type=jnp.float32).astype(jnp.bfloat16)

    moments = lax.map(leaf_moments, jnp.arange(LEAVES, dtype=jnp.int32))
    upward = [moments]
    fine_tables = []
    for level in range(3):
        transfer = fine_level(transfer_fine, row_count, firsts[level], counts[level])
        blocks = fine_level(couple_fine, row_count, firsts[level], counts[level])
        partners = fine_level(far_fine, row_count, firsts[level], counts[level])
        fine_tables.append((transfer, blocks, partners))
        moments = lift(moments, transfer)
        upward.append(moments)
    clusters = 2 * row_count
    depth = clusters.bit_length() - 3
    coarse_up = [moments]
    for step in range(depth):
        moments = lift(moments, transfer_coarse[clusters:2 * clusters])
        clusters = clusters // 2
        coarse_up.append(moments)
    downward = moments
    for step in range(depth + 1):
        coupled = couple(coarse_up[depth - step], couple_coarse[clusters:2 * clusters], far_coarse[clusters:2 * clusters])
        if step == 0:
            downward = coupled.astype(jnp.bfloat16)
        else:
            downward = lower(downward, transfer_coarse[clusters:2 * clusters], coupled)
        clusters = clusters * 2
    for level in (2, 1, 0):
        transfer, blocks, partners = fine_tables[level]
        coupled = couple(upward[level], blocks, partners)
        downward = lower(downward, transfer, coupled)

    def leaf_output(index):
        summed = jnp.dot(target_basis[index], downward[index], preferred_element_type=jnp.float32)
        for slot in range(3):
            summed = summed + jnp.dot(near_blocks[index, slot], shaped[near_list[index, slot]], preferred_element_type=jnp.float32)
        return summed.astype(jnp.bfloat16)

    result = lax.map(leaf_output, jnp.arange(LEAVES, dtype=jnp.int32))
    return result.reshape(LEAVES * LEAF, width)
```

```python
import jax
import jax.numpy as jnp
from jax import lax
from jax.experimental import pallas as pl
from jax.experimental.pallas import tpu as pltpu
from jax.sharding import PartitionSpec as P

MESH = pl.DeviceIdType.MESH
F32 = jnp.float32
BF16 = jnp.bfloat16
MIB = 1024 * 1024


def dot(a, b):
    return lax.dot_general(a, b, (((1,), (0,)), ((), ())), preferred_element_type=F32)


def dot_t(a, b):
    return lax.dot_general(a, b, (((0,), (0,)), ((), ())), preferred_element_type=F32)


def kernel(
    dims,
    x_hbm,
    near_hbm,
    near_list_hbm,
    sb_hbm,
    tb_hbm,
    ef_hbm,
    ec_hbm,
    sf_hbm,
    sc_hbm,
    far_fine_hbm,
    far_coarse_hbm,
    part,
    tt,
    f0,
    top,
    near_list,
    far_fine,
    far_coarse,
    xw,
    near,
    sb,
    tb,
    ef,
    ec,
    sf,
    sc,
    wf,
    wc,
    cw0,
    cw1,
    cw2,
    cw3,
    cr,
    cu,
    f3,
    f2,
    f1,
    edge_sum,
    lifts,
    q1,
    q0,
    load_sem,
    edge_send,
    edge_recv,
    halo_send,
    halo_recv,
    table_send,
    table_recv,
    gather_send,
    gather_recv,
    pair_send,
    pair_recv,
    lift_send,
    lift_recv,
    hello,
):
    count, leaf, rank, R, T, spans, pieces = dims
    me = lax.axis_index("rows")
    z = lax.axis_index("rhs")
    right, left = lax.rem(me + 1, R), lax.rem(me + R - 1, R)
    parity = lax.rem(me, 2)
    twin = me + 1 - 2 * parity
    block = ec.shape[0]
    sizes = [count, count // 2, count // 4, count // 8]
    firsts = [0, count, count + count // 2]
    windows = [cw0, cw1, cw2, cw3]

    def load(source, target, k):
        copy = pltpu.make_async_copy(source, target, load_sem.at[k])
        copy.start()
        return copy

    barrier = pltpu.get_barrier_semaphore()
    for k in range(1, R):
        pl.semaphore_signal(
            barrier, inc=1, device_id=(lax.rem(me + k, R), z), device_id_type=MESH
        )
    for k in range(1, T):

        @pl.when(z + k < T)
        def _():
            pl.semaphore_signal(barrier, inc=1, device_id=(me, z + k), device_id_type=MESH)

    edge_loads = [
        load(x_hbm.at[pl.ds(0, 1)], xw.at[pl.ds(1, 1)], 0),
        load(x_hbm.at[pl.ds(count - 1, 1)], xw.at[pl.ds(count, 1)], 1),
    ]
    load_sb = load(sb_hbm, sb, 2)
    x_loads = [
        load(x_hbm.at[pl.ds(a, b - a)], xw.at[pl.ds(1 + a, b - a)], 16 + c)
        for c, (a, b) in enumerate(spans)
    ]
    load_ef = load(ef_hbm, ef, 3)
    load_ec = load(ec_hbm, ec, 4)
    load_sc = load(sc_hbm, sc, 5)
    load_lists = [
        load(near_list_hbm, near_list, 6),
        load(far_fine_hbm, far_fine, 7),
        load(far_coarse_hbm, far_coarse, 8),
    ]

    def send(src, dst, send_sem, recv_sem, row, col):
        return pltpu.make_async_remote_copy(
            src_ref=src,
            dst_ref=dst,
            send_sem=send_sem,
            recv_sem=recv_sem,
            device_id=(row, col),
            device_id_type=MESH,
        )

    def both(low_src, low_dst, high_src, high_dst, send_sem, recv_sem, k):
        low = send(low_src, low_dst, send_sem.at[2 * k], recv_sem.at[2 * k], left, z)
        high = send(high_src, high_dst, send_sem.at[2 * k + 1], recv_sem.at[2 * k + 1], right, z)
        low.start()
        high.start()
        return [low, high]

    for copy in edge_loads:
        copy.wait()
    pl.semaphore_wait(barrier, R - 1 + z)
    for k in range(1, T):

        @pl.when(z >= k)
        def _():
            pl.semaphore_signal(hello, inc=1, device_id=(me, z - k), device_id_type=MESH)

    rows = leaf // pieces

    def edge_piece(k):
        span = pl.ds(k * rows, rows)
        return both(
            xw.at[1, span],
            xw.at[count + 1, span],
            xw.at[count, span],
            xw.at[0, span],
            edge_send,
            edge_recv,
            k,
        )

    edges = [edge_piece(k) for k in range(pieces // 2)]

    load_sb.wait()

    def leaf_moment(t):
        cw0[2 + t] = dot(sb[t], xw[1 + t]).astype(BF16)

    leaf_moment(0)
    leaf_moment(count - 1)
    for c, (a, b) in enumerate(spans):
        x_loads[c].wait()
        for t in range(a, b):
            leaf_moment(t)
    load_near = load(near_hbm, near, 9)
    load_sf = load(sf_hbm, sf, 10)
    load_tb = load(tb_hbm, tb, 11)

    load_ef.wait()

    def pair_matrix(level, j):
        first = firsts[level] + 2 * j
        return ef[first : first + 2].reshape(2 * rank, rank)

    low_pack = [pair_matrix(level, 0) for level in range(3)]
    high_pack = [pair_matrix(level, sizes[level + 1] - 1) for level in range(3)]
    lifts[0] = jnp.concatenate(low_pack + low_pack[:1], axis=1)
    lifts[1] = jnp.concatenate(high_pack + high_pack[:1], axis=1)

    halos = [None] * 4
    for level in range(3):
        below, above = windows[level], windows[level + 1]
        for j in range(sizes[level + 1]):
            pair = below[2 + 2 * j : 4 + 2 * j].reshape(2 * rank, -1)
            above[2 + j] = dot_t(pair_matrix(level, j), pair).astype(BF16)
        if level == 0:
            tables = both(
                lifts.at[0], lifts.at[3], lifts.at[1], lifts.at[2], lift_send, lift_recv, 0
            )
            halos[0] = both(
                cw0.at[pl.ds(2, 2)],
                cw0.at[pl.ds(2 + count, 2)],
                cw0.at[pl.ds(count, 2)],
                cw0.at[pl.ds(0, 2)],
                halo_send,
                halo_recv,
                0,
            )

    def inner_halo(level):
        ref, size = windows[level], sizes[level]
        return both(
            ref.at[pl.ds(3, 1)],
            ref.at[pl.ds(size + 3, 1)],
            ref.at[pl.ds(size, 1)],
            ref.at[pl.ds(0, 1)],
            halo_send,
            halo_recv,
            level,
        )

    load_ec.wait()
    load_sc.wait()
    for r in range(block):
        wc[z * block + r] = jnp.concatenate([sc[r, 0], sc[r, 1], sc[r, 2], ec[r]], axis=1)
    for level in (1, 2, 3):
        halos[level] = inner_halo(level)
    edges += [edge_piece(k) for k in range(pieces // 2, pieces)]

    pair_rows = wc.at[pl.ds(2 * R + 2 * me, 2)]
    pair_owner = (2 * R + 2 * me) // block
    coarse_blocks = (2 * R + block - 1) // block
    mine = wc.at[pl.ds(z * block, block)]

    def pair_copy(k, source, target):
        return send(pair_rows, pair_rows, pair_send.at[k], pair_recv.at[source], me, target)

    def table_copy(k, source, target):
        return send(mine, mine, table_send.at[k], table_recv.at[source], me, target)

    for copy in load_lists:
        copy.wait()
    total = count * R

    def near_term(t, wanted):
        target = lax.rem(me * count + t + wanted + total, total)
        slot = jnp.where(
            near_list[0, t] == target, 0, jnp.where(near_list[1, t] == target, 1, 2)
        )
        return dot(near[t, slot], xw[1 + t + wanted])

    def near_leaf(t):
        part[t] = (near_term(t, -1) + near_term(t, 0) + near_term(t, 1)).astype(BF16)

    def near_step(i, carry):
        for u in range(2):
            near_leaf(1 + 2 * i + u)
        return carry

    steps = (count - 2) // 2
    load_near.wait()

    @pl.when(z > 0)
    def _():
        @pl.when(z == pair_owner)
        def _():
            for k in range(1, T):

                @pl.when(z >= k)
                def _():
                    pair_copy(k, z, z - k).start()

        @pl.when(z < coarse_blocks)
        def _():
            for k in range(1, T):

                @pl.when(z >= k)
                def _():
                    table_copy(k, z, z - k).start()

    lax.fori_loop(0, steps // 2, near_step, 0)

    @pl.when(z < T - 1)
    def _():
        pl.semaphore_wait(hello, T - 1 - z)

    @pl.when(z == pair_owner)
    def _():
        for k in range(1, T):

            @pl.when(z < k)
            def _():
                pair_copy(k, z, lax.rem(z - k + T, T)).start()

    @pl.when(z < coarse_blocks)
    def _():
        for k in range(1, T):

            @pl.when(z < k)
            def _():
                table_copy(k, z, lax.rem(z - k + T, T)).start()

    lax.fori_loop(steps // 2, steps, near_step, 0)

    @pl.when(z != pair_owner)
    def _():
        pair_copy(0, pair_owner, lax.rem(z + 1, T)).wait_recv()

    def transfer(row):
        return wc[row][:, 3 * rank :]

    own = dot_t(transfer(2 * R + 2 * me), cw3[2]) + dot_t(transfer(2 * R + 2 * me + 1), cw3[3])
    cr[me] = own.astype(BF16)

    def gather_copy(source, target, k):
        spot = cr.at[pl.ds(source, 1)]
        return send(spot, spot, gather_send.at[k], gather_recv.at[source], target, z)

    gathers = []
    for k in range(1, R // 2):
        gathers.append(gather_copy(me, lax.rem(me + 2 * k, R), k))
    gathers.append(gather_copy(me, twin, 0))
    for copy in gathers:
        copy.start()

    edge_sum[0] = near_term(0, 0) + near_term(0, 1)
    edge_sum[1] = near_term(count - 1, -1) + near_term(count - 1, 0)

    load_sf.wait()
    for j in range(wf.shape[0]):
        wf[j] = jnp.concatenate([sf[j, 0], sf[j, 1], sf[j, 2], ef[j]], axis=1)

    for j in range(sizes[2]):
        both_rows = dot(pair_matrix(1, j), ef[firsts[2] + j]).astype(BF16)
        q1[2 * j : 2 * j + 2] = both_rows.reshape(2, rank, rank)
    for j in range(sizes[1]):
        both_rows = dot(pair_matrix(0, j), q1[j]).astype(BF16)
        q0[2 * j : 2 * j + 2] = both_rows.reshape(2, rank, rank)
    across = lax.broadcasted_iota(jnp.int32, (rank, rank), 0)
    down = lax.broadcasted_iota(jnp.int32, (rank, rank), 1)
    unit = jnp.where(across == down, 1.0, 0.0).astype(BF16)
    load_tb.wait()
    for t in range(count):
        tt[t] = dot_t(tb[t], jnp.concatenate([unit, q0[t]], axis=1)).astype(BF16)

    for copy in tables:
        copy.wait_recv()
    for copy in halos[0]:
        copy.wait_recv()
    for level in range(3):
        below, above = windows[level], windows[level + 1]
        size = sizes[level]
        for copy in halos[level + 1]:
            copy.wait_recv()
        from_left = lifts[2][:, level * rank : (level + 1) * rank]
        from_right = lifts[3][:, level * rank : (level + 1) * rank]
        low_pair = below[0:2].reshape(2 * rank, -1)
        high_pair = below[size + 2 : size + 4].reshape(2 * rank, -1)
        above[1] = dot_t(from_left, low_pair).astype(BF16)
        above[size // 2 + 2] = dot_t(from_right, high_pair).astype(BF16)

    for i in range(2):
        row = 2 * R + 2 * me + i
        parts = [
            cw3[jnp.minimum(lax.rem(far_coarse[s, row] - 2 * me + 2 + 2 * R, 2 * R), 5)]
            for s in range(3)
        ]
        f3[i] = dot(wc[row][:, : 3 * rank], jnp.concatenate(parts, axis=0)).astype(BF16)
    upper = f3
    for level, below in ((2, f2), (1, f1), (0, f0)):
        m = sizes[level]
        n = m * R
        for i in range(m):
            row = firsts[level] + i
            parts = [
                windows[level][jnp.minimum(lax.rem(far_fine[s, row] - m * me + 2 + n, n), m + 3)]
                for s in range(3)
            ] + [upper[i // 2]]
            below[i] = dot(wf[row], jnp.concatenate(parts, axis=0)).astype(BF16)
        upper = below

    forwards = []
    for k in range(1, R // 2):
        other = lax.rem(me + 2 * k, R)
        gather_copy(other, me, k).wait_recv()
        copy = gather_copy(other, twin, R // 2 + k)
        copy.start()
        forwards.append(copy)

    for pair in edges:
        for copy in pair:
            copy.wait_recv()
    part[0] = (edge_sum[0] + near_term(0, -1)).astype(BF16)
    part[count - 1] = (edge_sum[1] + near_term(count - 1, 1)).astype(BF16)

    for k in range(R // 2):
        other = lax.rem(twin + 2 * k, R)
        gather_copy(other, me, 0).wait_recv()
    for k in range(1, T):
        other = lax.rem(z + k, T)
        theirs = wc.at[pl.ds(other * block, block)]

        @pl.when(other < coarse_blocks)
        def _():
            send(theirs, theirs, table_send.at[0], table_recv.at[other], me, other).wait_recv()

    def coarse(n, index):
        return cr[index] if n == R else cu[n - 4 + index]

    n = R // 2
    while n >= 4:
        for j in range(n):
            lifted = dot_t(transfer(2 * n + 2 * j), coarse(2 * n, 2 * j)) + dot_t(
                transfer(2 * n + 2 * j + 1), coarse(2 * n, 2 * j + 1)
            )
            cu[n - 4 + j] = lifted.astype(BF16)
        n //= 2
    n = 4
    value = None
    while n <= R:
        row = n + me // (R // n)
        if n == 4:
            value = dot(wc[row][:, :rank], coarse(n, far_coarse[0, row]))
        else:
            parts = [coarse(n, far_coarse[s, row]) for s in range(3)] + [value]
            value = dot(wc[row], jnp.concatenate(parts, axis=0))
        value = value.astype(BF16)
        n *= 2
    for i in range(2):
        top[i] = dot(transfer(2 * R + 2 * me + i), value).astype(BF16)

    @pl.when(z == pair_owner)
    def _():
        for k in range(1, T):
            pair_copy(k, z, lax.rem(z - k + T, T)).wait_send()

    @pl.when(z < coarse_blocks)
    def _():
        for k in range(1, T):
            table_copy(k, z, lax.rem(z - k + T, T)).wait_send()

    for copy in gathers + forwards + tables:
        copy.wait_send()
    for pair in halos + edges:
        for copy in pair:
            copy.wait_send()


def finish(part, tt, f, top, out_hbm, out, sem):
    count = part.shape[0]
    stores = []
    for t in range(count):
        moments = jnp.concatenate([f[t], top[t * top.shape[0] // count]], axis=0)
        out[t] = (part[t].astype(F32) + dot(tt[t], moments)).astype(BF16)
        copy = pltpu.make_async_copy(out.at[t], out_hbm.at[t], sem.at[t])
        copy.start()
        stores.append(copy)
    for copy in stores:
        copy.wait()


def body(
    sources,
    near_blocks,
    near_list,
    source_basis,
    target_basis,
    transfer_fine,
    transfer_coarse,
    couple_fine,
    couple_coarse,
    far_fine,
    far_coarse,
):
    count, _, leaf, _ = near_blocks.shape
    rank = source_basis.shape[2]
    width = sources.shape[1]
    R, T = lax.axis_size("rows"), lax.axis_size("rhs")
    fine = transfer_fine.shape[0]
    block = transfer_coarse.shape[0]
    cuts = [1, 1 + (count - 2) // 4, count // 2, count - 1 - (count - 2) // 4, count - 1]
    spans = list(zip(cuts[:-1], cuts[1:]))
    pieces = 4
    dims = (count, leaf, rank, R, T, spans, pieces)
    hbm = pl.BlockSpec(memory_space=pltpu.HBM)
    vmem = pl.BlockSpec(memory_space=pltpu.VMEM)

    def in_hbm(a):
        return pltpu.with_memory_space_constraint(a, pltpu.HBM)

    def moments(clusters):
        return pltpu.VMEM((clusters, rank, width), BF16)

    dma = pltpu.SemaphoreType.DMA
    target = in_hbm(jnp.swapaxes(target_basis, 1, 2))
    results = pl.pallas_call(
        lambda *refs: kernel(dims, *refs),
        name="tree_apply",
        out_shape=[
            pltpu.VMEM((count, leaf, width), BF16),
            pltpu.VMEM((count, leaf, 2 * rank), BF16),
            moments(count),
            moments(count // 8),
        ],
        in_specs=[hbm] * 11,
        out_specs=[vmem] * 4,
        scratch_shapes=[
            pltpu.SMEM(near_list.shape[::-1], jnp.int32),
            pltpu.SMEM(far_fine.shape[::-1], jnp.int32),
            pltpu.SMEM(far_coarse.shape[::-1], jnp.int32),
            pltpu.VMEM((count + 2, leaf, width), BF16),
            pltpu.VMEM(near_blocks.shape, BF16),
            pltpu.VMEM((count, rank, leaf), BF16),
            pltpu.VMEM((count, rank, leaf), BF16),
            pltpu.VMEM(transfer_fine.shape, BF16),
            pltpu.VMEM(transfer_coarse.shape, BF16),
            pltpu.VMEM(couple_fine.shape, BF16),
            pltpu.VMEM(couple_coarse.shape, BF16),
            pltpu.VMEM((fine, rank, 4 * rank), BF16),
            pltpu.VMEM((block * T, rank, 4 * rank), BF16),
            moments(count + 4),
            moments(count // 2 + 4),
            moments(count // 4 + 4),
            moments(count // 8 + 4),
            moments(R),
            moments(R),
            moments(count // 8),
            moments(count // 4),
            moments(count // 2),
            pltpu.VMEM((2, leaf, width), F32),
            pltpu.VMEM((4, 2 * rank, 4 * rank), BF16),
            pltpu.VMEM((count // 2, rank, rank), BF16),
            pltpu.VMEM((count, rank, rank), BF16),
            dma((16 + len(spans),)),
            dma((2 * pieces,)),
            dma((2 * pieces,)),
            dma((8,)),
            dma((8,)),
            dma((T,)),
            dma((T,)),
            dma((R,)),
            dma((R,)),
            dma((T,)),
            dma((T,)),
            dma((2,)),
            dma((2,)),
            pltpu.SemaphoreType.REGULAR,
        ],
        compiler_params=pltpu.CompilerParams(
            collective_id=0, has_side_effects=True, vmem_limit_bytes=40 * MIB
        ),
    )(
        in_hbm(sources.reshape(count, leaf, width)),
        in_hbm(near_blocks),
        in_hbm(near_list.T),
        in_hbm(jnp.swapaxes(source_basis, 1, 2)),
        target,
        in_hbm(transfer_fine),
        in_hbm(transfer_coarse),
        in_hbm(couple_fine),
        in_hbm(couple_coarse),
        in_hbm(far_fine.T),
        in_hbm(far_coarse.T),
    )
    out = pl.pallas_call(
        finish,
        name="far_add",
        out_shape=jax.ShapeDtypeStruct((count, leaf, width), BF16),
        in_specs=[vmem] * 4,
        out_specs=pl.BlockSpec(memory_space=pl.ANY),
        scratch_shapes=[pltpu.VMEM((count, leaf, width), BF16), dma((count,))],
        compiler_params=pltpu.CompilerParams(vmem_limit_bytes=20 * MIB),
    )(*results)
    return out.reshape(count * leaf, width)


def solution(mesh):
    in_specs = (
        P("rows", "rhs"),
        P("rows", None, None, None),
        P("rows", None),
        P("rows", None, None),
        P("rows", None, None),
        P("rows", None, None),
        P("rhs", None, None),
        P("rows", None, None, None),
        P("rhs", None, None, None),
        P("rows", None),
        P(),
    )
    out_specs = P("rows", "rhs")
    return jax.shard_map(body, mesh=mesh, in_specs=in_specs, out_specs=out_specs, check_vma=False)
```

```python
import jax
import jax.numpy as jnp
from jax import lax
from jax.experimental import pallas as pl
from jax.experimental.pallas import tpu as pltpu
from jax.sharding import PartitionSpec as P

MESH = pl.DeviceIdType.MESH
F32 = jnp.float32
BF16 = jnp.bfloat16
MIB = 1024 * 1024


def dot(a, b):
    return lax.dot_general(a, b, (((1,), (0,)), ((), ())), preferred_element_type=F32)


def dot_t(a, b):
    return lax.dot_general(a, b, (((0,), (0,)), ((), ())), preferred_element_type=F32)


def kernel(
    dims,
    x_hbm,
    near_hbm,
    near_list_hbm,
    sb_hbm,
    tb_hbm,
    ef_hbm,
    ec_hbm,
    sf_hbm,
    sc_hbm,
    far_fine_hbm,
    far_coarse_hbm,
    part,
    tt,
    f0,
    top,
    near_list,
    far_fine,
    far_coarse,
    xw,
    nears,
    near_edges,
    sb,
    tb,
    ef,
    sf,
    coarse_in,
    wf,
    wc,
    cw0,
    cw1,
    cw2,
    cw3,
    cr,
    cu,
    f3,
    f2,
    f1,
    edge_sum,
    lifts,
    q1,
    q0,
    load_sem,
    sent,
    edge_recv,
    halo_recv,
    table_recv,
    gather_recv,
    pair_recv,
    hello,
):
    count, leaf, rank, R, T, spans, pieces = dims
    me = lax.axis_index("rows")
    z = lax.axis_index("rhs")
    right, left = lax.rem(me + 1, R), lax.rem(me + R - 1, R)
    parity = lax.rem(me, 2)
    twin = me + 1 - 2 * parity
    block = coarse_in.shape[0]
    sizes = [count, count // 2, count // 4, count // 8]
    firsts = [0, count, count + count // 2]
    windows = [cw0, cw1, cw2, cw3]

    def whole(ref, sem):
        return pltpu.make_async_copy(ref, ref, sem)

    def load(source, target, k):
        copy = pltpu.make_async_copy(source, target, load_sem.at[k])
        copy.start()
        return copy

    barrier = pltpu.get_barrier_semaphore()
    for k in range(1, R):
        other = lax.rem(me + k, R)

        @pl.when((other > me) | (k in (1, R - 1)))
        def _():
            pl.semaphore_signal(barrier, inc=1, device_id=(other, z), device_id_type=MESH)

    for k in range(1, T):

        @pl.when(z + k < T)
        def _():
            pl.semaphore_signal(barrier, inc=1, device_id=(me, z + k), device_id_type=MESH)

    load(x_hbm.at[pl.ds(0, 1)], xw.at[pl.ds(1, 1)], 0)
    load(x_hbm.at[pl.ds(count - 1, 1)], xw.at[pl.ds(count, 1)], 0)
    load(ec_hbm, coarse_in.at[:, 3], 1)
    load(sc_hbm, coarse_in.at[:, pl.ds(0, 3)], 1)
    load_sb = load(sb_hbm, sb, 2)
    x_loads = [
        load(x_hbm.at[pl.ds(a, b - a)], xw.at[pl.ds(1 + a, b - a)], 7 + c)
        for c, (a, b) in enumerate(spans)
    ]
    load_ef = load(ef_hbm, ef, 3)
    load_lists = [
        load(near_list_hbm, near_list, 4),
        load(far_fine_hbm, far_fine, 5),
        load(far_coarse_hbm, far_coarse, 6),
    ]

    def send(src, dst, send_sem, recv_sem, row, col):
        return pltpu.make_async_remote_copy(
            src_ref=src,
            dst_ref=dst,
            send_sem=send_sem,
            recv_sem=recv_sem,
            device_id=(row, col),
            device_id_type=MESH,
        )

    def both(low_src, low_dst, high_src, high_dst, level):
        send(low_src, low_dst, sent.at[1], halo_recv.at[level], left, z).start()
        send(high_src, high_dst, sent.at[1], halo_recv.at[level], right, z).start()

    before = me - jnp.where(me > 0, 1, 0) - jnp.where(me == R - 1, 1, 0)
    pl.semaphore_wait(barrier, z + 2 + before)
    for k in range(2, R - 1):
        other = lax.rem(me + k, R)

        @pl.when(other < me)
        def _():
            pl.semaphore_signal(hello.at[0], inc=1, device_id=(other, z), device_id_type=MESH)

    for k in range(1, T):

        @pl.when(z >= k)
        def _():
            pl.semaphore_signal(hello.at[1], inc=1, device_id=(me, z - k), device_id_type=MESH)

    rows = leaf // pieces

    def edge_piece(k, source, first, last):
        span = pl.ds(k * rows, rows)
        low = send(
            source.at[first, span],
            xw.at[count + 1, span],
            sent.at[0],
            edge_recv.at[0],
            left,
            z,
        )
        high = send(
            source.at[last, span],
            xw.at[0, span],
            sent.at[0],
            edge_recv.at[0],
            right,
            z,
        )
        return [low, high]

    edges = [edge_piece(k, x_hbm, 0, count - 1) for k in range(pieces // 2)]
    for pair in edges:
        for copy in pair:
            copy.start()

    whole(coarse_in, load_sem.at[1]).wait()
    for r in range(block):
        wc[z * block + r] = jnp.concatenate([coarse_in[r, k] for k in range(4)], axis=1)
    compact = R == 8
    step = 1 - 2 * parity
    near_by = lax.rem(me - step + R, R)
    pair_owner = (2 * R + 2 * me) // block
    by_owner = (2 * R + 2 * near_by) // block
    coarse_blocks = (2 * R + block - 1) // block
    mine = wc.at[pl.ds(z * block, block)]

    def pair_copy(target):
        rows = wc.at[pl.ds(2 * R + 2 * me, 2)]
        return send(rows, rows, sent.at[2], pair_recv.at[0], me, target)

    def by_copy(target):
        rows = wc.at[pl.ds(2 * R + 2 * near_by, 2)]
        return send(rows, rows, sent.at[3], pair_recv.at[1], me, target)

    pair_copies = [(pair_owner, pair_copy)] + ([(by_owner, by_copy)] if compact else [])

    def table_copy(source, target):
        spot = jnp.minimum(source, coarse_blocks - 1)
        return send(mine, mine, sent.at[4], table_recv.at[spot], me, target)

    for owner, copy_of in pair_copies:

        @pl.when(z == owner)
        def _():
            for k in range(1, T):

                @pl.when(z >= k)
                def _():
                    copy_of(z - k).start()

    @pl.when((z > 0) & (z < coarse_blocks))
    def _():
        for k in range(1, T):

            @pl.when(z >= k)
            def _():
                table_copy(z, z - k).start()

    load_sb.wait()

    def leaf_moment(t):
        cw0[2 + t] = dot(sb[t], xw[1 + t]).astype(BF16)

    near_loads = []

    def load_near(c):
        if c < len(spans):
            span = pl.ds(spans[c][0], spans[c][1] - spans[c][0])
            return [load(near_hbm.at[span], nears[c], 7 + c)]
        return [
            load(near_hbm.at[pl.ds(t, 1)], near_edges.at[pl.ds(k, 1)], 0)
            for k, t in enumerate((0, count - 1))
        ]

    whole(xw.at[pl.ds(0, 2)], load_sem.at[0]).wait()
    leaf_moment(0)
    leaf_moment(count - 1)
    for c, (a, b) in enumerate(spans):
        x_loads[c].wait()
        near_loads.append(load_near(c))
        for t in range(a, b):
            leaf_moment(t)
    near_loads.append(load_near(len(spans)))
    load_sf = load(sf_hbm, sf, 2)
    load_tb = load(tb_hbm, tb, 1)

    early = (z == pair_owner) | (z == by_owner) if compact else z == pair_owner

    def hear_planes():
        @pl.when(z < T - 1)
        def _():
            pl.semaphore_wait(hello.at[1], T - 1 - z)

    @pl.when(early)
    def _():
        hear_planes()
        for owner, copy_of in pair_copies:

            @pl.when(z == owner)
            def _():
                for k in range(1, T):

                    @pl.when(z < T - k)
                    def _():
                        copy_of(z + k).start()

    load_ef.wait()

    def pair_matrix(level, j):
        first = firsts[level] + 2 * j
        return ef[first : first + 2].reshape(2 * rank, rank)

    low_pack = [pair_matrix(level, 0) for level in range(3)]
    high_pack = [pair_matrix(level, sizes[level + 1] - 1) for level in range(3)]
    lifts[0] = jnp.concatenate(low_pack + low_pack[:1], axis=1)
    lifts[1] = jnp.concatenate(high_pack + high_pack[:1], axis=1)

    for level in range(3):
        below, above = windows[level], windows[level + 1]
        for j in range(sizes[level + 1]):
            pair = below[2 + 2 * j : 4 + 2 * j].reshape(2 * rank, -1)
            above[2 + j] = dot_t(pair_matrix(level, j), pair).astype(BF16)
        if level == 0:
            both(lifts.at[0], lifts.at[3], lifts.at[1], lifts.at[2], 0)
            both(
                cw0.at[pl.ds(2, 2)],
                cw0.at[pl.ds(2 + count, 2)],
                cw0.at[pl.ds(count, 2)],
                cw0.at[pl.ds(0, 2)],
                0,
            )

    def inner_halo(level):
        ref, size = windows[level], sizes[level]
        both(
            ref.at[pl.ds(3, 1)],
            ref.at[pl.ds(size + 3, 1)],
            ref.at[pl.ds(size, 1)],
            ref.at[pl.ds(0, 1)],
            level,
        )

    for level in (1, 2, 3):
        inner_halo(level)

    for copy in load_lists:
        copy.wait()
    total = count * R

    def near_terms(t, near, at, first, last):
        blocks = []
        for wanted in range(first, last + 1):
            target = lax.rem(me * count + t + wanted + total, total)
            slot = jnp.where(
                near_list[0, t] == target, 0, jnp.where(near_list[1, t] == target, 1, 2)
            )
            blocks.append(near[at, slot])
        points = xw[1 + t + first : 2 + t + last].reshape(-1, xw.shape[2])
        return dot(jnp.concatenate(blocks, axis=1), points)

    def near_span(c):
        near_loads[c][0].wait()
        for t in range(*spans[c]):
            part[t] = near_terms(t, nears[c], t - spans[c][0], -1, 1).astype(BF16)


    for c in range(len(spans) // 2):
        near_span(c)

    @pl.when(jnp.logical_not(early))
    def _():
        hear_planes()

    @pl.when(z < coarse_blocks)
    def _():
        for k in range(1, T):

            @pl.when(z < T - k)
            def _():
                table_copy(z, z + k).start()

    for c in range(len(spans) // 2, len(spans)):
        near_span(c)

    def transfer(row):
        return wc[row][:, 3 * rank :]

    def coarse_moment(cluster, at):
        lower, upper = transfer(2 * R + 2 * cluster), transfer(2 * R + 2 * cluster + 1)
        cr[cluster] = (dot_t(lower, cw3[at]) + dot_t(upper, cw3[at + 1])).astype(BF16)

    def gather_copy(source, target, k):
        spot = cr.at[pl.ds(source, 1)]
        return send(spot, spot, sent.at[5], gather_recv.at[k], target, z)

    later = R - 1 - me - jnp.where(me == 0, 2, jnp.where(me == R - 1, 0, 1))

    @pl.when(later > 0)
    def _():
        pl.semaphore_wait(hello.at[0], later)

    @pl.when(z != pair_owner)
    def _():
        pair_copy(lax.rem(z + 1, T)).wait_recv()

    coarse_moment(me, 2)

    def ring(offset):
        return lax.rem(me + offset + 2 * R, R)

    if compact:
        targets = [(ring(2 * step), 0), (ring(R // 2), 1), (ring(R // 2 + step), 1)]
    else:
        targets = [(ring(2 * k), me) for k in range(1, R // 2)] + [(twin, me)]
    for target, k in targets:
        gather_copy(me, target, k).start()

    whole(near_edges, load_sem.at[0]).wait()
    edge_sum[0] = near_terms(0, near_edges, 0, 0, 1)
    edge_sum[1] = near_terms(count - 1, near_edges, 1, -1, 0)
    late = [edge_piece(k, xw, 1, count) for k in range(pieces // 2, pieces)]
    for pair in late:
        for copy in pair:
            copy.start()

    load_sf.wait()
    for j in range(wf.shape[0]):
        wf[j] = jnp.concatenate([sf[j, 0], sf[j, 1], sf[j, 2], ef[j]], axis=1)

    for j in range(sizes[2]):
        both_rows = dot(pair_matrix(1, j), ef[firsts[2] + j]).astype(BF16)
        q1[2 * j : 2 * j + 2] = both_rows.reshape(2, rank, rank)
    for j in range(sizes[1]):
        both_rows = dot(pair_matrix(0, j), q1[j]).astype(BF16)
        q0[2 * j : 2 * j + 2] = both_rows.reshape(2, rank, rank)
    across = lax.broadcasted_iota(jnp.int32, (rank, rank), 0)
    down = lax.broadcasted_iota(jnp.int32, (rank, rank), 1)
    unit = jnp.where(across == down, 1.0, 0.0).astype(BF16)
    load_tb.wait()
    for t in range(count):
        tt[t] = dot_t(tb[t], jnp.concatenate([unit, q0[t]], axis=1)).astype(BF16)

    whole(cw0.at[pl.ds(0, 5)], halo_recv.at[0]).wait()
    for level in range(3):
        below, above = windows[level], windows[level + 1]
        size = sizes[level]
        whole(cw0.at[pl.ds(0, 2)], halo_recv.at[level + 1]).wait()
        from_left = lifts[2][:, level * rank : (level + 1) * rank]
        from_right = lifts[3][:, level * rank : (level + 1) * rank]
        low_pair = below[0:2].reshape(2 * rank, -1)
        high_pair = below[size + 2 : size + 4].reshape(2 * rank, -1)
        above[1] = dot_t(from_left, low_pair).astype(BF16)
        above[size // 2 + 2] = dot_t(from_right, high_pair).astype(BF16)

    if compact:

        @pl.when(z != by_owner)
        def _():
            by_copy(lax.rem(z + 1, T)).wait_recv()

        coarse_moment(near_by, 4 * parity)
        gather_copy(near_by, twin, 2).start()

    for i in range(2):
        row = 2 * R + 2 * me + i
        parts = [
            cw3[jnp.minimum(lax.rem(far_coarse[s, row] - 2 * me + 2 + 2 * R, 2 * R), 5)]
            for s in range(3)
        ]
        f3[i] = dot(wc[row][:, : 3 * rank], jnp.concatenate(parts, axis=0)).astype(BF16)
    upper = f3
    for level, below in ((2, f2), (1, f1), (0, f0)):
        m = sizes[level]
        n = m * R
        for i in range(m):
            row = firsts[level] + i
            parts = [
                windows[level][jnp.minimum(lax.rem(far_fine[s, row] - m * me + 2 + n, n), m + 3)]
                for s in range(3)
            ] + [upper[i // 2]]
            below[i] = dot(wf[row], jnp.concatenate(parts, axis=0)).astype(BF16)
        upper = below

    if compact:
        beyond = ring(-2 * step)
        gather_copy(beyond, me, 0).wait_recv()
        gather_copy(beyond, twin, 2).start()
        whole(cr.at[pl.ds(0, 2)], gather_recv.at[1]).wait()
        whole(cr.at[pl.ds(0, 2)], gather_recv.at[2]).wait()
        passes = 5
    else:
        for k in range(1, R // 2):
            gather_copy(ring(2 * k), me, ring(2 * k)).wait_recv()
            gather_copy(ring(2 * k), twin, ring(2 * k)).start()
        for k in range(R // 2):
            other = lax.rem(twin + 2 * k, R)
            gather_copy(other, me, other).wait_recv()
        passes = R - 1
    for k in range(1, T):
        other = lax.rem(z + k, T)
        theirs = wc.at[pl.ds(other * block, block)]

        @pl.when(other < coarse_blocks)
        def _():
            spot = jnp.minimum(other, coarse_blocks - 1)
            send(theirs, theirs, sent.at[4], table_recv.at[spot], me, other).wait_recv()

    def coarse(n, index):
        return cr[index] if n == R else cu[n - 4 + index]

    def lift(n, j):
        lifted = dot_t(transfer(2 * n + 2 * j), coarse(2 * n, 2 * j)) + dot_t(
            transfer(2 * n + 2 * j + 1), coarse(2 * n, 2 * j + 1)
        )
        return lifted.astype(BF16)

    if not compact:
        n = R // 2
        while n >= 4:
            for j in range(n):
                cu[n - 4 + j] = lift(n, j)
            n //= 2
    n = 4
    value = None
    while n <= R:
        row = n + me // (R // n)
        if n == 4:
            opposite = lax.rem(me // (R // n) + 2, 4)
            moment = lift(4, opposite) if compact else coarse(4, opposite)
            value = dot(wc[row][:, :rank], moment)
        else:
            parts = [coarse(n, far_coarse[s, row]) for s in range(3)] + [value]
            value = dot(wc[row], jnp.concatenate(parts, axis=0))
        value = value.astype(BF16)
        n *= 2
    for i in range(2):
        top[i] = dot(transfer(2 * R + 2 * me + i), value).astype(BF16)

    whole(xw.at[pl.ds(0, 2)], edge_recv.at[0]).wait()
    part[0] = (edge_sum[0] + near_terms(0, near_edges, 0, -1, -1)).astype(BF16)
    part[count - 1] = (edge_sum[1] + near_terms(count - 1, near_edges, 1, 1, 1)).astype(BF16)

    for k, (owner, copy_of) in enumerate(pair_copies):

        @pl.when(z == owner)
        def _():
            whole(wc.at[pl.ds(0, 2 * (T - 1))], sent.at[2 + k]).wait()

    @pl.when(z < coarse_blocks)
    def _():
        whole(wc.at[pl.ds(0, block * (T - 1))], sent.at[4]).wait()

    whole(cr.at[pl.ds(0, passes)], sent.at[5]).wait()
    whole(xw.at[pl.ds(0, 2)], sent.at[0]).wait()
    whole(cw0.at[pl.ds(0, 11)], sent.at[1]).wait()


def finish(part, tt, f, top, out_hbm, out, sem):
    count = part.shape[0]
    for t in range(count):
        moments = jnp.concatenate([f[t], top[t * top.shape[0] // count]], axis=0)
        out[t] = (part[t].astype(F32) + dot(tt[t], moments)).astype(BF16)
        pltpu.make_async_copy(out.at[t], out_hbm.at[t], sem).start()
    pltpu.make_async_copy(out, out_hbm, sem).wait()


def body(
    sources,
    near_blocks,
    near_list,
    source_basis,
    target_basis,
    transfer_fine,
    transfer_coarse,
    couple_fine,
    couple_coarse,
    far_fine,
    far_coarse,
):
    count, _, leaf, _ = near_blocks.shape
    rank = source_basis.shape[2]
    width = sources.shape[1]
    R, T = lax.axis_size("rows"), lax.axis_size("rhs")
    fine = transfer_fine.shape[0]
    block = transfer_coarse.shape[0]
    cuts = [1, 1 + (count - 2) // 4, count // 2, count - 1 - (count - 2) // 4, count - 1]
    spans = list(zip(cuts[:-1], cuts[1:]))
    pieces = 4
    dims = (count, leaf, rank, R, T, spans, pieces)
    hbm = pl.BlockSpec(memory_space=pltpu.HBM)
    vmem = pl.BlockSpec(memory_space=pltpu.VMEM)

    def in_hbm(a):
        return pltpu.with_memory_space_constraint(a, pltpu.HBM)

    def moments(clusters):
        return pltpu.VMEM((clusters, rank, width), BF16)

    dma = pltpu.SemaphoreType.DMA
    target = in_hbm(jnp.swapaxes(target_basis, 1, 2))
    results = pl.pallas_call(
        lambda *refs: kernel(dims, *refs),
        name="tree_apply",
        out_shape=[
            pltpu.VMEM((count, leaf, width), BF16),
            pltpu.VMEM((count, leaf, 2 * rank), BF16),
            moments(count),
            moments(count // 8),
        ],
        in_specs=[hbm] * 11,
        out_specs=[vmem] * 4,
        scratch_shapes=[
            pltpu.SMEM(near_list.shape[::-1], jnp.int32),
            pltpu.SMEM(far_fine.shape[::-1], jnp.int32),
            pltpu.SMEM(far_coarse.shape[::-1], jnp.int32),
            pltpu.VMEM((count + 2, leaf, width), BF16),
            [pltpu.VMEM((b - a,) + near_blocks.shape[1:], BF16) for a, b in spans],
            pltpu.VMEM((2,) + near_blocks.shape[1:], BF16),
            pltpu.VMEM((count, rank, leaf), BF16),
            pltpu.VMEM((count, rank, leaf), BF16),
            pltpu.VMEM(transfer_fine.shape, BF16),
            pltpu.VMEM(couple_fine.shape, BF16),
            pltpu.VMEM((block, 4, rank, rank), BF16),
            pltpu.VMEM((fine, rank, 4 * rank), BF16),
            pltpu.VMEM((block * T, rank, 4 * rank), BF16),
            moments(count + 4),
            moments(count // 2 + 4),
            moments(count // 4 + 4),
            moments(count // 8 + 4),
            moments(R),
            moments(R),
            moments(count // 8),
            moments(count // 4),
            moments(count // 2),
            pltpu.VMEM((2, leaf, width), F32),
            pltpu.VMEM((4, 2 * rank, 4 * rank), BF16),
            pltpu.VMEM((count // 2, rank, rank), BF16),
            pltpu.VMEM((count, rank, rank), BF16),
            dma((7 + len(spans),)),
            dma((6,)),
            dma((1,)),
            dma((4,)),
            dma((2 * R // block,)),
            dma((3 if R == 8 else R,)),
            dma((2,)),
            pltpu.SemaphoreType.REGULAR((2,)),
        ],
        compiler_params=pltpu.CompilerParams(
            collective_id=0, has_side_effects=True, vmem_limit_bytes=40 * MIB
        ),
    )(
        in_hbm(sources.reshape(count, leaf, width)),
        in_hbm(near_blocks),
        in_hbm(near_list.T),
        in_hbm(jnp.swapaxes(source_basis, 1, 2)),
        target,
        in_hbm(transfer_fine),
        in_hbm(transfer_coarse),
        in_hbm(couple_fine),
        in_hbm(couple_coarse),
        in_hbm(far_fine.T),
        in_hbm(far_coarse.T),
    )
    out = pl.pallas_call(
        finish,
        name="far_add",
        out_shape=jax.ShapeDtypeStruct((count, leaf, width), BF16),
        in_specs=[vmem] * 4,
        out_specs=pl.BlockSpec(memory_space=pl.ANY),
        scratch_shapes=[pltpu.VMEM((count, leaf, width), BF16), dma],
        compiler_params=pltpu.CompilerParams(vmem_limit_bytes=20 * MIB),
    )(*results)
    return out.reshape(count * leaf, width)


def solution(mesh):
    in_specs = (
        P("rows", "rhs"),
        P("rows", None, None, None),
        P("rows", None),
        P("rows", None, None),
        P("rows", None, None),
        P("rows", None, None),
        P("rhs", None, None),
        P("rows", None, None, None),
        P("rhs", None, None, None),
        P("rows", None),
        P(),
    )
    out_specs = P("rows", "rhs")
    return jax.shard_map(body, mesh=mesh, in_specs=in_specs, out_specs=out_specs, check_vma=False)
```

```python
import jax
import jax.numpy as jnp
from jax import lax
from jax.experimental import pallas as pl
from jax.experimental.pallas import tpu as pltpu
from jax.sharding import PartitionSpec as P

MESH = pl.DeviceIdType.MESH
F32 = jnp.float32
BF16 = jnp.bfloat16
LEAD = 6
MIB = 1024 * 1024


def dot(a, b):
    return lax.dot_general(a, b, (((1,), (0,)), ((), ())), preferred_element_type=F32)


def dot_n(a, b):
    return lax.dot_general(a, b, (((1,), (1,)), ((), ())), preferred_element_type=F32)


def dot_t(a, b):
    return lax.dot_general(a, b, (((0,), (0,)), ((), ())), preferred_element_type=F32)


def kernel(
    dims,
    x_hbm,
    near_hbm,
    near_list_hbm,
    sb_hbm,
    tb_hbm,
    ef_hbm,
    ec_hbm,
    sf_hbm,
    sc_hbm,
    far_fine_hbm,
    far_coarse_hbm,
    part,
    tt,
    f0,
    top,
    edge_block,
    beyond_leaf,
    near_list,
    far_fine,
    far_coarse,
    xw,
    nears,
    near_edges,
    sb,
    tb,
    ef,
    sf,
    coarse_in,
    wf,
    wc,
    cw0,
    cw1,
    cw2,
    cw3,
    cr,
    cu,
    f3,
    f2,
    f1,
    lifts,
    q1,
    q0,
    load_sem,
    sent,
    edge_recv,
    halo_recv,
    table_recv,
    gather_recv,
    rows_recv,
    hello,
):
    count, leaf, rank, R, T, spans = dims
    me = lax.axis_index("rows")
    z = lax.axis_index("rhs")
    right, left = lax.rem(me + 1, R), lax.rem(me + R - 1, R)
    parity = lax.rem(me, 2)
    twin = me + 1 - 2 * parity
    block = coarse_in.shape[0]
    compact = R == 8
    halo_sent, gather_sent, rows_sent = (0, 0, 1) if compact else (1, 2, 4)
    sizes = [count, count // 2, count // 4, count // 8]
    firsts = [0, count, count + count // 2]
    windows = [cw0, cw1, cw2, cw3]

    def whole(ref, sem):
        return pltpu.make_async_copy(ref, ref, sem)

    def load(source, target, k):
        copy = pltpu.make_async_copy(source, target, load_sem.at[k])
        copy.start()
        return copy

    barrier = pltpu.get_barrier_semaphore()
    for k in range(1, R):
        other = lax.rem(me + k, R)

        @pl.when((other > me) | (k in (1, R - 1)))
        def _():
            pl.semaphore_signal(barrier, inc=1, device_id=(other, z), device_id_type=MESH)

    for k in range(1, T):

        @pl.when(z + k < T)
        def _():
            pl.semaphore_signal(barrier, inc=1, device_id=(me, z + k), device_id_type=MESH)

    load(x_hbm.at[pl.ds(0, 1)], xw.at[pl.ds(1, 1)], 0)
    load(x_hbm.at[pl.ds(count - 1, 1)], xw.at[pl.ds(count, 1)], 0)
    load(ec_hbm, coarse_in.at[:, 3], 1)
    load(sc_hbm, coarse_in.at[:, pl.ds(0, 3)], 1)
    load_sb = load(sb_hbm, sb, 2)
    x_loads = [
        load(x_hbm.at[pl.ds(a, b - a)], xw.at[pl.ds(1 + a, b - a)], 7 + c)
        for c, (a, b) in enumerate(spans)
    ]
    load_ef = load(ef_hbm, ef, 3)
    load_lists = [
        load(near_list_hbm, near_list, 4),
        load(far_fine_hbm, far_fine, 5),
        load(far_coarse_hbm, far_coarse, 6),
    ]

    def send(src, dst, send_sem, recv_sem, row, col):
        return pltpu.make_async_remote_copy(
            src_ref=src,
            dst_ref=dst,
            send_sem=send_sem,
            recv_sem=recv_sem,
            device_id=(row, col),
            device_id_type=MESH,
        )

    def both(low_src, low_dst, high_src, high_dst, level):
        send(low_src, low_dst, sent.at[halo_sent], halo_recv.at[min(level, 1)], left, z).start()
        send(high_src, high_dst, sent.at[halo_sent], halo_recv.at[min(level, 1)], right, z).start()

    step = 1 - 2 * parity
    near_by = lax.rem(me - step + R, R)
    coarse_blocks = (2 * R + block - 1) // block
    mine = wc.at[pl.ds(z * block, block)]

    opposite = lax.rem(me // 2 + 2, 4)
    row_sets = [(2 * R + 2 * me, 2)]
    if compact:
        row_sets += [(2 * R + 2 * near_by, 2), (R + me, 1), (R + 2 * opposite, 2), (4 + me // 2, 1)]

    def rows_copy(k, target):
        first, size = row_sets[k]
        rows = wc.at[pl.ds(first, size)]
        return send(rows, rows, sent.at[rows_sent + k], rows_recv.at[k], me, target)

    def owner(k):
        return row_sets[k][0] // block

    def send_rows(chosen, before):
        for k in chosen:

            @pl.when(z == owner(k))
            def _():
                for d in range(1, T):
                    target = z - d if before else z + d

                    @pl.when((target >= 0) & (target < T))
                    def _():
                        rows_copy(k, target).start()

    def receive_rows(chosen):
        for k in chosen:

            @pl.when(z != owner(k))
            def _():
                rows_copy(k, lax.rem(z + 1, T)).wait_recv()

    def send_tables(before):
        if not compact:

            @pl.when(z < coarse_blocks)
            def _():
                for d in range(1, T):
                    target = z - d if before else z + d

                    @pl.when((target >= 0) & (target < T))
                    def _():
                        spot = table_recv.at[z]
                        send(mine, mine, sent.at[3], spot, me, target).start()

    urgent = range(min(2, len(row_sets)))
    later_sets = range(len(urgent), len(row_sets))
    early = (z == owner(0)) | (z == owner(urgent[-1]))

    cut = leaf * LEAD // 8
    outward = jnp.where(parity == 0, left, right)
    leads = jnp.where(me < 2, parity == 0, outward < lax.rem(me + 2 * step + R, R))

    def send_edge(source, first, high, begin=0, end=leaf):
        at = first + (count - 1 if high else 0)
        span = pl.ds(begin, end - begin)
        landing = beyond_leaf.at[0 if high else 1, span]
        target = right if high else left
        send(source.at[at, span], landing, sent.at[0], edge_recv.at[0], target, z).start()

    def enter():
        before = me - jnp.where(me > 0, 1, 0) - jnp.where(me == R - 1, 1, 0)
        pl.semaphore_wait(barrier, z + 2 + before)
        for k in range(2, R - 1):
            other = lax.rem(me + k, R)

            @pl.when(other < me)
            def _():
                pl.semaphore_signal(
                    hello.at[0], inc=1, device_id=(other, z), device_id_type=MESH
                )

        for k in range(1, T):

            @pl.when(z >= k)
            def _():
                pl.semaphore_signal(hello.at[1], inc=1, device_id=(me, z - k), device_id_type=MESH)

        for high in (0, 1):

            @pl.when(parity != high)
            def _():
                send_edge(x_hbm, 0, high)

            @pl.when(leads & (parity == high))
            def _():
                send_edge(x_hbm, 0, high, 0, cut)


    def coarse_rows():
        whole(coarse_in, load_sem.at[1]).wait()
        for r in range(block):
            wc[z * block + r] = jnp.concatenate([coarse_in[r, k] for k in range(4)], axis=1)
        send_rows(range(len(row_sets)), True)
        send_tables(True)

    def hear_planes():
        @pl.when(z < T - 1)
        def _():
            pl.semaphore_wait(hello.at[1], T - 1 - z)

    def early_rows():
        @pl.when(early)
        def _():
            hear_planes()
            send_rows(urgent, False)

    near_loads = [
        pltpu.make_async_copy(near_hbm.at[pl.ds(a, b - a)], nears[c], load_sem.at[7 + c])
        for c, (a, b) in enumerate(spans)
    ]
    edge_loads = [
        pltpu.make_async_copy(near_hbm.at[pl.ds(t, 1)], near_edges.at[pl.ds(k, 1)], load_sem.at[0])
        for k, t in enumerate((0, count - 1))
    ]
    load_sf = pltpu.make_async_copy(sf_hbm, sf, load_sem.at[2])
    load_tb = pltpu.make_async_copy(tb_hbm, tb, load_sem.at[1])

    def leaf_moment(t):
        cw0[2 + t] = dot(sb[t], xw[1 + t]).astype(BF16)

    def moments():
        load_sb.wait()
        whole(xw.at[pl.ds(0, 2)], load_sem.at[0]).wait()
        leaf_moment(0)
        leaf_moment(count - 1)
        for c, (a, b) in enumerate(spans):
            x_loads[c].wait()
            near_loads[c].start()
            for t in range(a, b):
                leaf_moment(t)
        for copy in edge_loads + [load_sf]:
            copy.start()

    def pair_matrix(level, j):
        first = firsts[level] + 2 * j
        return ef[first : first + 2].reshape(2 * rank, rank)

    def halo(level):
        ref, size = windows[level], sizes[level]
        if level == 0:
            both(lifts.at[0], lifts.at[3], lifts.at[1], lifts.at[2], 0)
        width, at = (2, 2) if level == 0 else (1, 3)
        both(
            ref.at[pl.ds(at, width)],
            ref.at[pl.ds(size + at, width)],
            ref.at[pl.ds(size, width)],
            ref.at[pl.ds(0, width)],
            level,
        )

    def upward(sending):
        load_ef.wait()
        low_pack = [pair_matrix(level, 0) for level in range(3)]
        high_pack = [pair_matrix(level, sizes[level + 1] - 1) for level in range(3)]
        lifts[0] = jnp.concatenate(low_pack + low_pack[:1], axis=1)
        lifts[1] = jnp.concatenate(high_pack + high_pack[:1], axis=1)
        for level in range(3):
            below, above = windows[level], windows[level + 1]
            for j in range(sizes[level + 1]):
                pair = below[2 + 2 * j : 4 + 2 * j].reshape(2 * rank, -1)
                above[2 + j] = dot_t(pair_matrix(level, j), pair).astype(BF16)
            if level == 0 and sending:
                halo(0)

    first_chip = (me < 2) & (z == 0)

    @pl.when(first_chip)
    def _():
        moments()
        upward(False)
        enter()
        halo(0)

    @pl.when(jnp.logical_not(first_chip))
    def _():
        enter()
        coarse_rows()
        moments()
        early_rows()
        upward(True)

    for level in (1, 2, 3):
        halo(level)

    @pl.when(first_chip)
    def _():
        coarse_rows()
        early_rows()

    load_tb.start()
    for copy in load_lists:
        copy.wait()
    total = count * R

    def near_block(t, near, at, wanted):
        target = lax.rem(me * count + t + wanted + total, total)
        slot = jnp.where(
            near_list[0, t] == target, 0, jnp.where(near_list[1, t] == target, 1, 2)
        )
        return near[at, slot]

    def near_terms(t, near, at, first, last):
        blocks = [near_block(t, near, at, wanted) for wanted in range(first, last + 1)]
        points = xw[1 + t + first : 2 + t + last].reshape(-1, xw.shape[2])
        return dot(jnp.concatenate(blocks, axis=1), points)

    def near_span(c):
        near_loads[c].wait()
        for t in range(*spans[c]):
            part[t] = near_terms(t, nears[c], t - spans[c][0], -1, 1).astype(BF16)


    for c in range(len(spans)):
        near_span(c)

    def transfer(row):
        return wc[row][:, 3 * rank :]

    def coarse_moment(cluster, at):
        lower, upper = transfer(2 * R + 2 * cluster), transfer(2 * R + 2 * cluster + 1)
        cr[cluster] = (dot_t(lower, cw3[at]) + dot_t(upper, cw3[at + 1])).astype(BF16)

    def gather_copy(source, target, k):
        spot = cr.at[pl.ds(source, 1)]
        return send(spot, spot, sent.at[gather_sent], gather_recv.at[k], target, z)

    @pl.when(jnp.logical_not(early))
    def _():
        hear_planes()

    send_rows(later_sets, False)
    send_tables(False)
    later = R - 1 - me - jnp.where(me == 0, 2, jnp.where(me == R - 1, 0, 1))

    @pl.when(later > 0)
    def _():
        pl.semaphore_wait(hello.at[0], later)

    receive_rows(range(1))
    coarse_moment(me, 2)

    def ring(offset):
        return lax.rem(me + offset + 2 * R, R)

    if compact:
        targets = [(ring(2 * step), 0), (ring(R // 2), 1), (ring(R // 2 + step), 1)]
    else:
        targets = [(ring(2 * k), me) for k in range(1, R // 2)] + [(twin, me)]
    for target, k in targets:
        gather_copy(me, target, k).start()

    for high in (0, 1):

        @pl.when(leads & (parity == high))
        def _():
            send_edge(xw, 1, high, cut, leaf)

    whole(near_edges, load_sem.at[0]).wait()
    part[0] = near_terms(0, near_edges, 0, 0, 1).astype(BF16)
    part[count - 1] = near_terms(count - 1, near_edges, 1, -1, 0).astype(BF16)
    edge_block[0] = near_block(0, near_edges, 0, -1)
    edge_block[1] = near_block(count - 1, near_edges, 1, 1)

    load_sf.wait()
    for j in range(wf.shape[0]):
        wf[j] = jnp.concatenate([sf[j, 0], sf[j, 1], sf[j, 2], ef[j]], axis=1)

    for j in range(sizes[2]):
        both_rows = dot(pair_matrix(1, j), ef[firsts[2] + j]).astype(BF16)
        q1[2 * j : 2 * j + 2] = both_rows.reshape(2, rank, rank)
    for j in range(sizes[1]):
        both_rows = dot(pair_matrix(0, j), q1[j]).astype(BF16)
        q0[2 * j : 2 * j + 2] = both_rows.reshape(2, rank, rank)
    across = lax.broadcasted_iota(jnp.int32, (rank, rank), 0)
    down = lax.broadcasted_iota(jnp.int32, (rank, rank), 1)
    unit = jnp.where(across == down, 1.0, 0.0).astype(BF16)
    load_tb.wait()
    for t in range(count):
        tt[t] = dot_t(tb[t], jnp.concatenate([unit, q0[t]], axis=1)).astype(BF16)

    for high in (0, 1):

        @pl.when(jnp.logical_not(leads | first_chip) & (parity == high))
        def _():
            send_edge(xw, 1, high)

    whole(cw0.at[pl.ds(0, 5)], halo_recv.at[0]).wait()
    for level in range(3):
        below, above = windows[level], windows[level + 1]
        size = sizes[level]
        if level == 0:
            whole(cw0.at[pl.ds(0, 6)], halo_recv.at[1]).wait()
        from_left = lifts[2][:, level * rank : (level + 1) * rank]
        from_right = lifts[3][:, level * rank : (level + 1) * rank]
        low_pair = below[0:2].reshape(2 * rank, -1)
        high_pair = below[size + 2 : size + 4].reshape(2 * rank, -1)
        above[1] = dot_t(from_left, low_pair).astype(BF16)
        above[size // 2 + 2] = dot_t(from_right, high_pair).astype(BF16)

    for high in (0, 1):

        @pl.when(jnp.logical_not(leads) & first_chip & (parity == high))
        def _():
            send_edge(xw, 1, high)

    if compact:

        receive_rows(range(1, 2))
        coarse_moment(near_by, 4 * parity)
        gather_copy(near_by, twin, 2).start()

    for i in range(2):
        row = 2 * R + 2 * me + i
        parts = [
            cw3[jnp.minimum(lax.rem(far_coarse[s, row] - 2 * me + 2 + 2 * R, 2 * R), 5)]
            for s in range(3)
        ]
        f3[i] = dot(wc[row][:, : 3 * rank], jnp.concatenate(parts, axis=0)).astype(BF16)
    upper = f3
    for level, below in ((2, f2), (1, f1), (0, f0)):
        m = sizes[level]
        n = m * R
        for i in range(m):
            row = firsts[level] + i
            parts = [
                windows[level][jnp.minimum(lax.rem(far_fine[s, row] - m * me + 2 + n, n), m + 3)]
                for s in range(3)
            ] + [upper[i // 2]]
            below[i] = dot(wf[row], jnp.concatenate(parts, axis=0)).astype(BF16)
        upper = below

    receive_rows(later_sets)
    if not compact:
        for k in range(1, T):
            other = lax.rem(z + k, T)
            theirs = wc.at[pl.ds(other * block, block)]

            @pl.when(other < coarse_blocks)
            def _():
                spot = table_recv.at[other]
                send(theirs, theirs, sent.at[3], spot, me, other).wait_recv()

    def upper_rows():
        return jnp.concatenate([transfer(2 * R + 2 * me + i) for i in range(2)], axis=0)

    if compact:
        down = dot(upper_rows(), wc[R + me]).astype(BF16)
        across = wc[4 + me // 2][:, :rank]
        lifted = [dot_n(across, transfer(R + 2 * opposite + i)).astype(BF16) for i in range(2)]
        far_up = dot(down[:, 3 * rank :], jnp.concatenate(lifted, axis=1)).astype(BF16)
        coarse_matrix = jnp.concatenate([down[:, : 3 * rank], far_up], axis=1)

    if compact:
        beyond = ring(-2 * step)
        gather_copy(beyond, me, 0).wait_recv()
        gather_copy(beyond, twin, 2).start()
        whole(cr.at[pl.ds(0, 2)], gather_recv.at[1]).wait()
        whole(cr.at[pl.ds(0, 2)], gather_recv.at[2]).wait()
        passes = 5
    else:
        for k in range(1, R // 2):
            gather_copy(ring(2 * k), me, ring(2 * k)).wait_recv()
            gather_copy(ring(2 * k), twin, ring(2 * k)).start()
        for k in range(R // 2):
            other = lax.rem(twin + 2 * k, R)
            gather_copy(other, me, other).wait_recv()
        passes = R - 1
    def coarse(n, index):
        return cr[index] if n == R else cu[n - 4 + index]

    def lift(n, j):
        lifted = dot_t(transfer(2 * n + 2 * j), coarse(2 * n, 2 * j)) + dot_t(
            transfer(2 * n + 2 * j + 1), coarse(2 * n, 2 * j + 1)
        )
        return lifted.astype(BF16)

    if compact:
        parts = [cr[far_coarse[s, R + me]] for s in range(3)]
        parts += [cr[2 * opposite], cr[2 * opposite + 1]]
        pair = dot(coarse_matrix, jnp.concatenate(parts, axis=0))
    else:
        n = R // 2
        while n >= 4:
            for j in range(n):
                cu[n - 4 + j] = lift(n, j)
            n //= 2
        n = 4
        value = None
        while n <= R:
            row = n + me // (R // n)
            if n == 4:
                value = dot(wc[row][:, :rank], coarse(n, far_coarse[0, row]))
            else:
                parts = [coarse(n, far_coarse[s, row]) for s in range(3)] + [value]
                value = dot(wc[row], jnp.concatenate(parts, axis=0))
            value = value.astype(BF16)
            n *= 2
        pair = dot(upper_rows(), value)
    top[...] = pair.astype(BF16).reshape(top.shape)

    whole(xw.at[pl.ds(0, 2)], edge_recv.at[0]).wait()
    for k in range(len(row_sets)):

        @pl.when(z == owner(k))
        def _():
            whole(wc.at[pl.ds(0, row_sets[k][1] * (T - 1))], sent.at[rows_sent + k]).wait()

    if not compact:

        @pl.when(z < coarse_blocks)
        def _():
            whole(wc.at[pl.ds(0, block * (T - 1))], sent.at[3]).wait()

    if compact:
        leaves, over = divmod(2 * leaf + (11 + passes) * rank, leaf)
        assert over == 0
        whole(xw.at[pl.ds(0, leaves)], sent.at[0]).wait()
    else:
        whole(xw.at[pl.ds(0, 2)], sent.at[0]).wait()
        whole(cw0.at[pl.ds(0, 11)], sent.at[halo_sent]).wait()
        whole(cr.at[pl.ds(0, passes)], sent.at[gather_sent]).wait()


def finish(part, tt, f, top, edge_block, beyond_leaf, out_hbm, out, sem):
    count = part.shape[0]
    middle = count // 2
    order = [*range(1, middle), 0, count - 1, *range(middle, count - 1)]
    for t in order:
        matrix, rows = tt[t], jnp.concatenate([f[t], top[t * top.shape[0] // count]], axis=0)
        if t in (0, count - 1):
            matrix = jnp.concatenate([edge_block[t // (count - 1)], matrix], axis=1)
            rows = jnp.concatenate([beyond_leaf[t // (count - 1)], rows], axis=0)
        out[t] = (part[t].astype(F32) + dot(matrix, rows)).astype(BF16)
        pltpu.make_async_copy(out.at[t], out_hbm.at[t], sem).start()
    pltpu.make_async_copy(out, out_hbm, sem).wait()


def body(
    sources,
    near_blocks,
    near_list,
    source_basis,
    target_basis,
    transfer_fine,
    transfer_coarse,
    couple_fine,
    couple_coarse,
    far_fine,
    far_coarse,
):
    count, _, leaf, _ = near_blocks.shape
    rank = source_basis.shape[2]
    width = sources.shape[1]
    R, T = lax.axis_size("rows"), lax.axis_size("rhs")
    fine = transfer_fine.shape[0]
    block = transfer_coarse.shape[0]
    cuts = [1, 1 + (count - 2) // 4, count // 2, count - 1 - (count - 2) // 4, count - 1]
    spans = list(zip(cuts[:-1], cuts[1:]))
    dims = (count, leaf, rank, R, T, spans)
    hbm = pl.BlockSpec(memory_space=pltpu.HBM)
    vmem = pl.BlockSpec(memory_space=pltpu.VMEM)

    def in_hbm(a):
        return pltpu.with_memory_space_constraint(a, pltpu.HBM)

    def moments(clusters):
        return pltpu.VMEM((clusters, rank, width), BF16)

    dma = pltpu.SemaphoreType.DMA
    target = in_hbm(jnp.swapaxes(target_basis, 1, 2))
    results = pl.pallas_call(
        lambda *refs: kernel(dims, *refs),
        name="tree_apply",
        out_shape=[
            pltpu.VMEM((count, leaf, width), BF16),
            pltpu.VMEM((count, leaf, 2 * rank), BF16),
            moments(count),
            moments(count // 8),
            pltpu.VMEM((2, leaf, leaf), BF16),
            pltpu.VMEM((2, leaf, width), BF16),
        ],
        in_specs=[hbm] * 11,
        out_specs=[vmem] * 6,
        scratch_shapes=[
            pltpu.SMEM(near_list.shape[::-1], jnp.int32),
            pltpu.SMEM(far_fine.shape[::-1], jnp.int32),
            pltpu.SMEM(far_coarse.shape[::-1], jnp.int32),
            pltpu.VMEM((count + 2, leaf, width), BF16),
            [pltpu.VMEM((b - a,) + near_blocks.shape[1:], BF16) for a, b in spans],
            pltpu.VMEM((2,) + near_blocks.shape[1:], BF16),
            pltpu.VMEM((count, rank, leaf), BF16),
            pltpu.VMEM((count, rank, leaf), BF16),
            pltpu.VMEM(transfer_fine.shape, BF16),
            pltpu.VMEM(couple_fine.shape, BF16),
            pltpu.VMEM((block, 4, rank, rank), BF16),
            pltpu.VMEM((fine, rank, 4 * rank), BF16),
            pltpu.VMEM((block * T, rank, 4 * rank), BF16),
            moments(count + 4),
            moments(count // 2 + 4),
            moments(count // 4 + 4),
            moments(count // 8 + 4),
            moments(R),
            moments(R),
            moments(count // 8),
            moments(count // 4),
            moments(count // 2),
            pltpu.VMEM((4, 2 * rank, 4 * rank), BF16),
            pltpu.VMEM((count // 2, rank, rank), BF16),
            pltpu.VMEM((count, rank, rank), BF16),
            dma((7 + len(spans),)),
            dma((6 if R == 8 else 5,)),
            dma((1,)),
            dma((2,)),
            dma((1 if R == 8 else T,)),
            dma((3 if R == 8 else R,)),
            dma((5 if R == 8 else 1,)),
            pltpu.SemaphoreType.REGULAR((2,)),
        ],
        compiler_params=pltpu.CompilerParams(
            collective_id=0, has_side_effects=True, vmem_limit_bytes=40 * MIB
        ),
    )(
        in_hbm(sources.reshape(count, leaf, width)),
        in_hbm(near_blocks),
        in_hbm(near_list.T),
        in_hbm(jnp.swapaxes(source_basis, 1, 2)),
        target,
        in_hbm(transfer_fine),
        in_hbm(transfer_coarse),
        in_hbm(couple_fine),
        in_hbm(couple_coarse),
        in_hbm(far_fine.T),
        in_hbm(far_coarse.T),
    )
    out = pl.pallas_call(
        finish,
        name="far_add",
        out_shape=jax.ShapeDtypeStruct((count, leaf, width), BF16),
        in_specs=[vmem] * 6,
        out_specs=pl.BlockSpec(memory_space=pl.ANY),
        scratch_shapes=[pltpu.VMEM((count, leaf, width), BF16), dma],
        compiler_params=pltpu.CompilerParams(vmem_limit_bytes=20 * MIB),
    )(*results)
    return out.reshape(count * leaf, width)


def solution(mesh):
    in_specs = (
        P("rows", "rhs"),
        P("rows", None, None, None),
        P("rows", None),
        P("rows", None, None),
        P("rows", None, None),
        P("rows", None, None),
        P("rhs", None, None),
        P("rows", None, None, None),
        P("rhs", None, None, None),
        P("rows", None),
        P(),
    )
    out_specs = P("rows", "rhs")
    return jax.shard_map(body, mesh=mesh, in_specs=in_specs, out_specs=out_specs, check_vma=False)
```

```python
import jax
import jax.numpy as jnp
from jax import lax
from jax.experimental import pallas as pl
from jax.experimental.pallas import tpu as pltpu
from jax.sharding import PartitionSpec as P

MESH = pl.DeviceIdType.MESH
F32 = jnp.float32
BF16 = jnp.bfloat16
LEAD = 6
TRAIL = 4
MIB = 1024 * 1024


def dot(a, b):
    return lax.dot_general(a, b, (((1,), (0,)), ((), ())), preferred_element_type=F32)


def dot_n(a, b):
    return lax.dot_general(a, b, (((1,), (1,)), ((), ())), preferred_element_type=F32)


def dot_t(a, b):
    return lax.dot_general(a, b, (((0,), (0,)), ((), ())), preferred_element_type=F32)


def kernel(
    dims,
    x_hbm,
    near_hbm,
    near_list_hbm,
    sb_hbm,
    tb_hbm,
    ef_hbm,
    ec_hbm,
    sf_hbm,
    sc_hbm,
    far_fine_hbm,
    far_coarse_hbm,
    part,
    tt,
    f0,
    top,
    edge_block,
    beyond_leaf,
    near_list,
    far_fine,
    far_coarse,
    xw,
    nears,
    near_edges,
    sb,
    tb,
    ef,
    sf,
    coarse_in,
    wf,
    wc,
    cw0,
    cw1,
    cw2,
    cw3,
    cr,
    cu,
    f3,
    f2,
    f1,
    lifts,
    q1,
    q0,
    load_sem,
    sent,
    edge_recv,
    halo_recv,
    gather_recv,
    rows_recv,
    hello,
):
    count, leaf, rank, R, T, spans = dims
    me = lax.axis_index("rows")
    z = lax.axis_index("rhs")
    right, left = lax.rem(me + 1, R), lax.rem(me + R - 1, R)
    parity = lax.rem(me, 2)
    twin = me + 1 - 2 * parity
    block = coarse_in.shape[0]
    compact = R == 8
    halo_sent, gather_sent, rows_sent = (0, 0, 1) if compact else (1, 2, 4)
    sizes = [count, count // 2, count // 4, count // 8]
    firsts = [0, count, count + count // 2]
    windows = [cw0, cw1, cw2, cw3]

    def whole(ref, sem):
        return pltpu.make_async_copy(ref, ref, sem)

    def load(source, target, k):
        copy = pltpu.make_async_copy(source, target, load_sem.at[k])
        copy.start()
        return copy

    barrier = pltpu.get_barrier_semaphore()
    for k in range(1, R):
        other = lax.rem(me + k, R)

        @pl.when((k in (1, R - 1)) | ((other > me) & (not compact)))
        def _():
            pl.semaphore_signal(barrier, inc=1, device_id=(other, z), device_id_type=MESH)

    for k in range(1, T):

        @pl.when(z + k < T)
        def _():
            pl.semaphore_signal(barrier, inc=1, device_id=(me, z + k), device_id_type=MESH)

    load(x_hbm.at[pl.ds(0, 1)], xw.at[pl.ds(1, 1)], 0)
    load(x_hbm.at[pl.ds(count - 1, 1)], xw.at[pl.ds(count, 1)], 0)
    load(ec_hbm, coarse_in.at[:, 3], 1)
    load(sc_hbm, coarse_in.at[:, pl.ds(0, 3)], 1)
    load_sb = load(sb_hbm, sb, 2)
    x_loads = [
        load(x_hbm.at[pl.ds(a, b - a)], xw.at[pl.ds(1 + a, b - a)], 7 + c)
        for c, (a, b) in enumerate(spans)
    ]
    load_ef = load(ef_hbm, ef, 3)
    load_lists = [
        load(near_list_hbm, near_list, 4),
        load(far_fine_hbm, far_fine, 5),
        load(far_coarse_hbm, far_coarse, 6),
    ]

    def send(src, dst, send_sem, recv_sem, row, col):
        return pltpu.make_async_remote_copy(
            src_ref=src,
            dst_ref=dst,
            send_sem=send_sem,
            recv_sem=recv_sem,
            device_id=(row, col),
            device_id_type=MESH,
        )

    def both(low_src, low_dst, high_src, high_dst, level):
        send(low_src, low_dst, sent.at[halo_sent], halo_recv.at[min(level, 1)], left, z).start()
        send(high_src, high_dst, sent.at[halo_sent], halo_recv.at[min(level, 1)], right, z).start()

    step = 1 - 2 * parity
    near_by = lax.rem(me - step + R, R)
    coarse_blocks = (2 * R + block - 1) // block
    mine = wc.at[pl.ds(z * block, block)]

    opposite = lax.rem(me // 2 + 2, 4)
    row_sets = [(2 * R + 2 * me, 2)]
    if compact:
        row_sets += [(2 * R + 2 * near_by, 2), (R + me, 1), (R + 2 * opposite, 2), (4 + me // 2, 1)]

    def rows_copy(k, target):
        first, size = row_sets[k]
        rows = wc.at[pl.ds(first, size)]
        return send(rows, rows, sent.at[rows_sent + k], rows_recv.at[k], me, target)

    def owner(k):
        return row_sets[k][0] // block

    def send_rows(chosen, before):
        for k in chosen:

            @pl.when(z == owner(k))
            def _():
                for d in range(1, T):
                    target = z - d if before else z + d

                    @pl.when((target >= 0) & (target < T))
                    def _():
                        rows_copy(k, target).start()

    def receive_rows(chosen):
        for k in chosen:

            @pl.when(z != owner(k))
            def _():
                rows_copy(k, lax.rem(z + 1, T)).wait_recv()

    def send_tables(before):
        if not compact:

            @pl.when(z < coarse_blocks)
            def _():
                for d in range(1, T):
                    target = z - d if before else z + d

                    @pl.when((target >= 0) & (target < T))
                    def _():
                        spot = rows_recv.at[1 + z]
                        send(mine, mine, sent.at[3], spot, me, target).start()

    urgent = range(min(2, len(row_sets)))
    later_sets = range(len(urgent), len(row_sets))
    early = (z == owner(0)) | (z == owner(urgent[-1]))

    cut = leaf * LEAD // 8
    outward = jnp.where(parity == 0, left, right)
    leads = jnp.where((me < 2) & (z == 0), parity == 0, outward < lax.rem(me + 2 * step + R, R))

    def send_edge(source, first, high, begin=0, end=leaf):
        at = first + (count - 1 if high else 0)
        span = pl.ds(begin, end - begin)
        landing = beyond_leaf.at[0 if high else 1, span]
        target = right if high else left
        send(source.at[at, span], landing, sent.at[0], edge_recv.at[0], target, z).start()

    rounds = [0, 2, 3]

    def tell(k):
        for other in (left, right):
            pl.semaphore_signal(
                hello.at[rounds[k]], inc=1, device_id=(other, z), device_id_type=MESH
            )

    def hear(k):
        pl.semaphore_wait(hello.at[rounds[k]], 2)

    def pass_on(k):
        if compact:
            hear(k)
            tell(k + 1)

    def enter():
        if compact:
            pl.semaphore_wait(barrier, z + 2)
            tell(0)
        else:
            before = me - jnp.where(me > 0, 1, 0) - jnp.where(me == R - 1, 1, 0)
            pl.semaphore_wait(barrier, z + 2 + before)
            for k in range(2, R - 1):
                other = lax.rem(me + k, R)

                @pl.when(other < me)
                def _():
                    pl.semaphore_signal(
                        hello.at[0], inc=1, device_id=(other, z), device_id_type=MESH
                    )

        for k in range(1, T):

            @pl.when(z >= k)
            def _():
                pl.semaphore_signal(hello.at[1], inc=1, device_id=(me, z - k), device_id_type=MESH)

        for high in (0, 1):

            @pl.when(parity != high)
            def _():
                send_edge(x_hbm, 0, high)

            @pl.when(leads & (parity == high))
            def _():
                send_edge(x_hbm, 0, high, 0, cut)


    def coarse_rows():
        whole(coarse_in, load_sem.at[1]).wait()
        for r in range(block):
            wc[z * block + r] = jnp.concatenate([coarse_in[r, k] for k in range(4)], axis=1)
        send_rows(range(len(row_sets)), True)
        send_tables(True)

    def hear_planes():
        @pl.when(z < T - 1)
        def _():
            pl.semaphore_wait(hello.at[1], T - 1 - z)

    def early_rows():
        @pl.when(early)
        def _():
            hear_planes()
            send_rows(urgent, False)

    near_loads = [
        pltpu.make_async_copy(near_hbm.at[pl.ds(a, b - a)], nears[c], load_sem.at[7 + c])
        for c, (a, b) in enumerate(spans)
    ]
    edge_loads = [
        pltpu.make_async_copy(near_hbm.at[pl.ds(t, 1)], near_edges.at[pl.ds(k, 1)], load_sem.at[0])
        for k, t in enumerate((0, count - 1))
    ]
    load_sf = pltpu.make_async_copy(sf_hbm, sf, load_sem.at[2])
    load_tb = pltpu.make_async_copy(tb_hbm, tb, load_sem.at[1])

    def leaf_moment(t):
        cw0[2 + t] = dot(sb[t], xw[1 + t]).astype(BF16)

    def moments():
        load_sb.wait()
        whole(xw.at[pl.ds(0, 2)], load_sem.at[0]).wait()
        leaf_moment(0)
        leaf_moment(count - 1)
        for c, (a, b) in enumerate(spans):
            x_loads[c].wait()
            near_loads[c].start()
            for t in range(a, b):
                leaf_moment(t)
        for copy in edge_loads + [load_sf]:
            copy.start()

    def pair_matrix(level, j):
        first = firsts[level] + 2 * j
        return ef[first : first + 2].reshape(2 * rank, rank)

    def halo(level):
        ref, size = windows[level], sizes[level]
        if level == 0:
            both(lifts.at[0], lifts.at[3], lifts.at[1], lifts.at[2], 0)
        width, at = (2, 2) if level == 0 else (1, 3)
        both(
            ref.at[pl.ds(at, width)],
            ref.at[pl.ds(size + at, width)],
            ref.at[pl.ds(size, width)],
            ref.at[pl.ds(0, width)],
            level,
        )

    def upward(sending):
        load_ef.wait()
        low_pack = [pair_matrix(level, 0) for level in range(3)]
        high_pack = [pair_matrix(level, sizes[level + 1] - 1) for level in range(3)]
        lifts[0] = jnp.concatenate(low_pack + low_pack[:1], axis=1)
        lifts[1] = jnp.concatenate(high_pack + high_pack[:1], axis=1)
        for level in range(3):
            below, above = windows[level], windows[level + 1]
            for j in range(sizes[level + 1]):
                pair = below[2 + 2 * j : 4 + 2 * j].reshape(2 * rank, -1)
                above[2 + j] = dot_t(pair_matrix(level, j), pair).astype(BF16)
            if level == 0 and sending:
                halo(0)

    first_chip = (me < 2) & (z == 0)

    @pl.when(first_chip)
    def _():
        moments()
        upward(False)
        enter()
        halo(0)

    @pl.when(jnp.logical_not(first_chip))
    def _():
        enter()
        coarse_rows()
        moments()
        early_rows()
        pass_on(0)
        upward(True)

    for level in (1, 2, 3):
        halo(level)

    @pl.when(first_chip)
    def _():
        coarse_rows()
        early_rows()

    load_tb.start()
    for copy in load_lists:
        copy.wait()
    total = count * R

    def near_block(t, near, at, wanted):
        target = lax.rem(me * count + t + wanted + total, total)
        slot = jnp.where(
            near_list[0, t] == target, 0, jnp.where(near_list[1, t] == target, 1, 2)
        )
        return near[at, slot]

    def near_terms(t, near, at, first, last):
        blocks = [near_block(t, near, at, wanted) for wanted in range(first, last + 1)]
        points = xw[1 + t + first : 2 + t + last].reshape(-1, xw.shape[2])
        return dot(jnp.concatenate(blocks, axis=1), points)

    def near_span(c):
        near_loads[c].wait()
        for t in range(*spans[c]):
            part[t] = near_terms(t, nears[c], t - spans[c][0], -1, 1).astype(BF16)


    for c in range(len(spans)):
        near_span(c)
        if c == 0:

            @pl.when(jnp.logical_not(first_chip))
            def _():
                pass_on(1)

        if c < 2:

            @pl.when(first_chip)
            def _():
                pass_on(c)


    def transfer(row):
        return wc[row][:, 3 * rank :]

    def coarse_moment(cluster, at):
        lower, upper = transfer(2 * R + 2 * cluster), transfer(2 * R + 2 * cluster + 1)
        cr[cluster] = (dot_t(lower, cw3[at]) + dot_t(upper, cw3[at + 1])).astype(BF16)

    def gather_copy(source, target, k):
        spot = cr.at[pl.ds(source, 1)]
        return send(spot, spot, sent.at[gather_sent], gather_recv.at[k], target, z)

    @pl.when(jnp.logical_not(early))
    def _():
        hear_planes()

    send_rows(later_sets, False)
    send_tables(False)
    if compact:
        hear(2)
    else:
        later = R - 1 - me - jnp.where(me == 0, 2, jnp.where(me == R - 1, 0, 1))

        @pl.when(later > 0)
        def _():
            pl.semaphore_wait(hello.at[0], later)

    receive_rows(range(1))
    coarse_moment(me, 2)

    def ring(offset):
        return lax.rem(me + offset + 2 * R, R)

    if compact:
        targets = [(ring(2 * step), 0), (ring(R // 2), 1), (ring(R // 2 + step), 1)]
    else:
        targets = [(ring(2 * k), me) for k in range(1, R // 2)] + [(twin, me)]
    for target, k in targets:
        gather_copy(me, target, k).start()

    for high in (0, 1):

        @pl.when(leads & (parity == high))
        def _():
            send_edge(xw, 1, high, cut, leaf)

    for high in (0, 1):

        @pl.when(jnp.logical_not(leads | first_chip) & (parity == high))
        def _():
            send_edge(xw, 1, high, 0, TRAIL * leaf // 8)

    whole(near_edges, load_sem.at[0]).wait()
    part[0] = near_terms(0, near_edges, 0, 0, 1).astype(BF16)
    part[count - 1] = near_terms(count - 1, near_edges, 1, -1, 0).astype(BF16)
    edge_block[0] = near_block(0, near_edges, 0, -1)
    edge_block[1] = near_block(count - 1, near_edges, 1, 1)

    load_sf.wait()
    for j in range(wf.shape[0]):
        wf[j] = jnp.concatenate([sf[j, 0], sf[j, 1], sf[j, 2], ef[j]], axis=1)

    for j in range(sizes[2]):
        both_rows = dot(pair_matrix(1, j), ef[firsts[2] + j]).astype(BF16)
        q1[2 * j : 2 * j + 2] = both_rows.reshape(2, rank, rank)
    for j in range(sizes[1]):
        both_rows = dot(pair_matrix(0, j), q1[j]).astype(BF16)
        q0[2 * j : 2 * j + 2] = both_rows.reshape(2, rank, rank)
    across = lax.broadcasted_iota(jnp.int32, (rank, rank), 0)
    down = lax.broadcasted_iota(jnp.int32, (rank, rank), 1)
    unit = jnp.where(across == down, 1.0, 0.0).astype(BF16)
    load_tb.wait()
    for t in range(count):
        tt[t] = dot_t(tb[t], jnp.concatenate([unit, q0[t]], axis=1)).astype(BF16)

    for high in (0, 1):

        @pl.when(jnp.logical_not(leads | first_chip) & (parity == high))
        def _():
            send_edge(xw, 1, high, TRAIL * leaf // 8, leaf)

    whole(cw0.at[pl.ds(0, 5)], halo_recv.at[0]).wait()
    for level in range(3):
        below, above = windows[level], windows[level + 1]
        size = sizes[level]
        if level == 0:
            whole(cw0.at[pl.ds(0, 6)], halo_recv.at[1]).wait()
        from_left = lifts[2][:, level * rank : (level + 1) * rank]
        from_right = lifts[3][:, level * rank : (level + 1) * rank]
        low_pair = below[0:2].reshape(2 * rank, -1)
        high_pair = below[size + 2 : size + 4].reshape(2 * rank, -1)
        above[1] = dot_t(from_left, low_pair).astype(BF16)
        above[size // 2 + 2] = dot_t(from_right, high_pair).astype(BF16)

    for high in (0, 1):

        @pl.when(jnp.logical_not(leads) & first_chip & (parity == high))
        def _():
            send_edge(xw, 1, high)

    if compact:

        receive_rows(range(1, 2))
        coarse_moment(near_by, 4 * parity)
        gather_copy(near_by, twin, 1).start()

    for i in range(2):
        row = 2 * R + 2 * me + i
        parts = [
            cw3[jnp.minimum(lax.rem(far_coarse[s, row] - 2 * me + 2 + 2 * R, 2 * R), 5)]
            for s in range(3)
        ]
        f3[i] = dot(wc[row][:, : 3 * rank], jnp.concatenate(parts, axis=0)).astype(BF16)
    upper = f3
    for level, below in ((2, f2), (1, f1), (0, f0)):
        m = sizes[level]
        n = m * R
        for i in range(m):
            row = firsts[level] + i
            parts = [
                windows[level][jnp.minimum(lax.rem(far_fine[s, row] - m * me + 2 + n, n), m + 3)]
                for s in range(3)
            ] + [upper[i // 2]]
            below[i] = dot(wf[row], jnp.concatenate(parts, axis=0)).astype(BF16)
        upper = below

    receive_rows(later_sets)
    if not compact:
        for k in range(1, T):
            other = lax.rem(z + k, T)
            theirs = wc.at[pl.ds(other * block, block)]

            @pl.when(other < coarse_blocks)
            def _():
                spot = rows_recv.at[1 + other]
                send(theirs, theirs, sent.at[3], spot, me, other).wait_recv()

    def upper_rows():
        return jnp.concatenate([transfer(2 * R + 2 * me + i) for i in range(2)], axis=0)

    if compact:
        down = dot(upper_rows(), wc[R + me]).astype(BF16)
        across = wc[4 + me // 2][:, :rank]
        lifted = [dot_n(across, transfer(R + 2 * opposite + i)).astype(BF16) for i in range(2)]
        far_up = dot(down[:, 3 * rank :], jnp.concatenate(lifted, axis=1)).astype(BF16)
        coarse_matrix = jnp.concatenate([down[:, : 3 * rank], far_up], axis=1)

    if compact:
        beyond = ring(-2 * step)
        gather_copy(beyond, me, 0).wait_recv()
        gather_copy(beyond, twin, 1).start()
        whole(cr.at[pl.ds(0, 4)], gather_recv.at[1]).wait()
        passes = 5
    else:
        for k in range(1, R // 2):
            gather_copy(ring(2 * k), me, ring(2 * k)).wait_recv()
            gather_copy(ring(2 * k), twin, ring(2 * k)).start()
        for k in range(R // 2):
            other = lax.rem(twin + 2 * k, R)
            gather_copy(other, me, other).wait_recv()
        passes = R - 1
    def coarse(n, index):
        return cr[index] if n == R else cu[n - 4 + index]

    def lift(n, j):
        lifted = dot_t(transfer(2 * n + 2 * j), coarse(2 * n, 2 * j)) + dot_t(
            transfer(2 * n + 2 * j + 1), coarse(2 * n, 2 * j + 1)
        )
        return lifted.astype(BF16)

    if compact:
        parts = [cr[far_coarse[s, R + me]] for s in range(3)]
        parts += [cr[2 * opposite], cr[2 * opposite + 1]]
        pair = dot(coarse_matrix, jnp.concatenate(parts, axis=0))
    else:
        n = R // 2
        while n >= 4:
            for j in range(n):
                cu[n - 4 + j] = lift(n, j)
            n //= 2
        n = 4
        value = None
        while n <= R:
            row = n + me // (R // n)
            if n == 4:
                value = dot(wc[row][:, :rank], coarse(n, far_coarse[0, row]))
            else:
                parts = [coarse(n, far_coarse[s, row]) for s in range(3)] + [value]
                value = dot(wc[row], jnp.concatenate(parts, axis=0))
            value = value.astype(BF16)
            n *= 2
        pair = dot(upper_rows(), value)
    top[...] = pair.astype(BF16).reshape(top.shape)

    whole(xw.at[pl.ds(0, 2)], edge_recv.at[0]).wait()
    for k in range(len(row_sets)):

        @pl.when(z == owner(k))
        def _():
            whole(wc.at[pl.ds(0, row_sets[k][1] * (T - 1))], sent.at[rows_sent + k]).wait()

    if not compact:

        @pl.when(z < coarse_blocks)
        def _():
            whole(wc.at[pl.ds(0, block * (T - 1))], sent.at[3]).wait()

    if compact:
        leaves, over = divmod(2 * leaf + (11 + passes) * rank, leaf)
        assert over == 0
        whole(xw.at[pl.ds(0, leaves)], sent.at[0]).wait()
    else:
        whole(xw.at[pl.ds(0, 2)], sent.at[0]).wait()
        whole(cw0.at[pl.ds(0, 11)], sent.at[halo_sent]).wait()
        whole(cr.at[pl.ds(0, passes)], sent.at[gather_sent]).wait()


def finish(part, tt, f, top, edge_block, beyond_leaf, out_hbm, out, sem):
    count = part.shape[0]
    middle = count // 2
    order = [*range(1, middle), 0, count - 1, *range(middle, count - 1)]
    for t in order:
        matrix, rows = tt[t], jnp.concatenate([f[t], top[t * top.shape[0] // count]], axis=0)
        if t in (0, count - 1):
            matrix = jnp.concatenate([edge_block[t // (count - 1)], matrix], axis=1)
            rows = jnp.concatenate([beyond_leaf[t // (count - 1)], rows], axis=0)
        out[t] = (part[t].astype(F32) + dot(matrix, rows)).astype(BF16)
        pltpu.make_async_copy(out.at[t], out_hbm.at[t], sem).start()
    pltpu.make_async_copy(out, out_hbm, sem).wait()


def body(
    sources,
    near_blocks,
    near_list,
    source_basis,
    target_basis,
    transfer_fine,
    transfer_coarse,
    couple_fine,
    couple_coarse,
    far_fine,
    far_coarse,
):
    count, _, leaf, _ = near_blocks.shape
    rank = source_basis.shape[2]
    width = sources.shape[1]
    R, T = lax.axis_size("rows"), lax.axis_size("rhs")
    fine = transfer_fine.shape[0]
    block = transfer_coarse.shape[0]
    cuts = [1, 1 + (count - 2) // 4, count // 2, count - 1 - (count - 2) // 4, count - 1]
    spans = list(zip(cuts[:-1], cuts[1:]))
    dims = (count, leaf, rank, R, T, spans)
    hbm = pl.BlockSpec(memory_space=pltpu.HBM)
    vmem = pl.BlockSpec(memory_space=pltpu.VMEM)

    def in_hbm(a):
        return pltpu.with_memory_space_constraint(a, pltpu.HBM)

    def moments(clusters):
        return pltpu.VMEM((clusters, rank, width), BF16)

    dma = pltpu.SemaphoreType.DMA
    target = in_hbm(jnp.swapaxes(target_basis, 1, 2))
    results = pl.pallas_call(
        lambda *refs: kernel(dims, *refs),
        name="tree_apply",
        out_shape=[
            pltpu.VMEM((count, leaf, width), BF16),
            pltpu.VMEM((count, leaf, 2 * rank), BF16),
            moments(count),
            moments(count // 8),
            pltpu.VMEM((2, leaf, leaf), BF16),
            pltpu.VMEM((2, leaf, width), BF16),
        ],
        in_specs=[hbm] * 11,
        out_specs=[vmem] * 6,
        scratch_shapes=[
            pltpu.SMEM(near_list.shape[::-1], jnp.int32),
            pltpu.SMEM(far_fine.shape[::-1], jnp.int32),
            pltpu.SMEM(far_coarse.shape[::-1], jnp.int32),
            pltpu.VMEM((count + 2, leaf, width), BF16),
            [pltpu.VMEM((b - a,) + near_blocks.shape[1:], BF16) for a, b in spans],
            pltpu.VMEM((2,) + near_blocks.shape[1:], BF16),
            pltpu.VMEM((count, rank, leaf), BF16),
            pltpu.VMEM((count, rank, leaf), BF16),
            pltpu.VMEM(transfer_fine.shape, BF16),
            pltpu.VMEM(couple_fine.shape, BF16),
            pltpu.VMEM((block, 4, rank, rank), BF16),
            pltpu.VMEM((fine, rank, 4 * rank), BF16),
            pltpu.VMEM((block * T, rank, 4 * rank), BF16),
            moments(count + 4),
            moments(count // 2 + 4),
            moments(count // 4 + 4),
            moments(count // 8 + 4),
            moments(R),
            moments(R),
            moments(count // 8),
            moments(count // 4),
            moments(count // 2),
            pltpu.VMEM((4, 2 * rank, 4 * rank), BF16),
            pltpu.VMEM((count // 2, rank, rank), BF16),
            pltpu.VMEM((count, rank, rank), BF16),
            dma((7 + len(spans),)),
            dma((6 if R == 8 else 5,)),
            dma((1,)),
            dma((2,)),
            dma((2 if R == 8 else R,)),
            dma((5 if R == 8 else 1 + T,)),
            pltpu.SemaphoreType.REGULAR((4 if R == 8 else 2,)),
        ],
        compiler_params=pltpu.CompilerParams(
            collective_id=0, has_side_effects=True, vmem_limit_bytes=40 * MIB
        ),
    )(
        in_hbm(sources.reshape(count, leaf, width)),
        in_hbm(near_blocks),
        in_hbm(near_list.T),
        in_hbm(jnp.swapaxes(source_basis, 1, 2)),
        target,
        in_hbm(transfer_fine),
        in_hbm(transfer_coarse),
        in_hbm(couple_fine),
        in_hbm(couple_coarse),
        in_hbm(far_fine.T),
        in_hbm(far_coarse.T),
    )
    out = pl.pallas_call(
        finish,
        name="far_add",
        out_shape=jax.ShapeDtypeStruct((count, leaf, width), BF16),
        in_specs=[vmem] * 6,
        out_specs=pl.BlockSpec(memory_space=pl.ANY),
        scratch_shapes=[pltpu.VMEM((count, leaf, width), BF16), dma],
        compiler_params=pltpu.CompilerParams(vmem_limit_bytes=20 * MIB),
    )(*results)
    return out.reshape(count * leaf, width)


def solution(mesh):
    in_specs = (
        P("rows", "rhs"),
        P("rows", None, None, None),
        P("rows", None),
        P("rows", None, None),
        P("rows", None, None),
        P("rows", None, None),
        P("rhs", None, None),
        P("rows", None, None, None),
        P("rhs", None, None, None),
        P("rows", None),
        P(),
    )
    out_specs = P("rows", "rhs")
    return jax.shard_map(body, mesh=mesh, in_specs=in_specs, out_specs=out_specs, check_vma=False)
```

```python
import jax
import jax.numpy as jnp
from jax import lax
from jax.experimental import pallas as pl
from jax.experimental.pallas import tpu as pltpu
from jax.sharding import PartitionSpec as P

MESH = pl.DeviceIdType.MESH
F32 = jnp.float32
BF16 = jnp.bfloat16
LEAD = 6
TRAIL = 4
MIB = 1024 * 1024


def dot(a, b):
    return lax.dot_general(a, b, (((1,), (0,)), ((), ())), preferred_element_type=F32)


def dot_n(a, b):
    return lax.dot_general(a, b, (((1,), (1,)), ((), ())), preferred_element_type=F32)


def dot_t(a, b):
    return lax.dot_general(a, b, (((0,), (0,)), ((), ())), preferred_element_type=F32)


def kernel(
    dims,
    x_hbm,
    near_hbm,
    near_list_hbm,
    sb_hbm,
    tb_hbm,
    ef_hbm,
    ec_hbm,
    sf_hbm,
    sc_hbm,
    far_fine_hbm,
    far_coarse_hbm,
    part,
    tt,
    f0,
    top,
    edge_block,
    beyond_leaf,
    near_list,
    far_fine,
    far_coarse,
    xw,
    nears,
    near_edges,
    sb,
    tb,
    ef,
    sf,
    coarse_in,
    wf,
    wc,
    cw0,
    cw1,
    cw2,
    cw3,
    cr,
    cu,
    f3,
    f2,
    f1,
    lifts,
    q1,
    q0,
    load_sem,
    sent,
    edge_recv,
    halo_recv,
    gather_recv,
    rows_recv,
    hello,
):
    count, leaf, rank, R, T, spans = dims
    me = lax.axis_index("rows")
    z = lax.axis_index("rhs")
    right, left = lax.rem(me + 1, R), lax.rem(me + R - 1, R)
    parity = lax.rem(me, 2)
    twin = me + 1 - 2 * parity
    block = coarse_in.shape[0]
    compact = R == 8
    halo_sent, gather_sent, rows_sent = (0, 0, 1) if compact else (1, 2, 4)
    sizes = [count, count // 2, count // 4, count // 8]
    firsts = [0, count, count + count // 2]
    windows = [cw0, cw1, cw2, cw3]

    def whole(ref, sem):
        return pltpu.make_async_copy(ref, ref, sem)

    def load(source, target, k):
        copy = pltpu.make_async_copy(source, target, load_sem.at[k])
        copy.start()
        return copy

    barrier = pltpu.get_barrier_semaphore()
    for k in range(1, R):
        other = lax.rem(me + k, R)

        @pl.when((k in (1, R - 1)) | ((other > me) & (not compact)))
        def _():
            pl.semaphore_signal(barrier, inc=1, device_id=(other, z), device_id_type=MESH)

    for k in range(1, T):

        @pl.when(z + k < T)
        def _():
            pl.semaphore_signal(barrier, inc=1, device_id=(me, z + k), device_id_type=MESH)

    load(x_hbm.at[pl.ds(0, 1)], xw.at[pl.ds(1, 1)], 0)
    load(x_hbm.at[pl.ds(count - 1, 1)], xw.at[pl.ds(count, 1)], 0)
    load(ec_hbm, coarse_in.at[:, 3], 1)
    load(sc_hbm, coarse_in.at[:, pl.ds(0, 3)], 1)
    load_sb = load(sb_hbm, sb, 2)
    x_loads = [
        load(x_hbm.at[pl.ds(a, b - a)], xw.at[pl.ds(1 + a, b - a)], 5 + c)
        for c, (a, b) in enumerate(spans)
    ]
    load_ef = load(ef_hbm, ef, 3)
    load_lists = [
        load(near_list_hbm, near_list, 4),
    ]

    def send(src, dst, send_sem, recv_sem, row, col):
        return pltpu.make_async_remote_copy(
            src_ref=src,
            dst_ref=dst,
            send_sem=send_sem,
            recv_sem=recv_sem,
            device_id=(row, col),
            device_id_type=MESH,
        )

    def both(low_src, low_dst, high_src, high_dst, level):
        send(low_src, low_dst, sent.at[halo_sent], halo_recv.at[min(level, 1)], left, z).start()
        send(high_src, high_dst, sent.at[halo_sent], halo_recv.at[min(level, 1)], right, z).start()

    step = 1 - 2 * parity
    near_by = lax.rem(me - step + R, R)
    coarse_blocks = (2 * R + block - 1) // block
    mine = wc.at[pl.ds(z * block, block)]

    opposite = lax.rem(me // 2 + 2, 4)
    row_sets = [(2 * R + 2 * me, 2)]
    if compact:
        row_sets += [(2 * R + 2 * near_by, 2), (R + me, 1), (R + 2 * opposite, 2), (4 + me // 2, 1)]

    def rows_copy(k, target):
        first, size = row_sets[k]
        rows = wc.at[pl.ds(first, size)]
        return send(rows, rows, sent.at[rows_sent + k], rows_recv.at[k], me, target)

    def owner(k):
        return row_sets[k][0] // block

    def send_rows(chosen, before):
        for k in chosen:

            @pl.when(z == owner(k))
            def _():
                for d in range(1, T):
                    target = z - d if before else z + d

                    @pl.when((target >= 0) & (target < T))
                    def _():
                        rows_copy(k, target).start()

    def receive_rows(chosen):
        for k in chosen:

            @pl.when(z != owner(k))
            def _():
                rows_copy(k, lax.rem(z + 1, T)).wait_recv()

    def send_tables(before):
        if not compact:

            @pl.when(z < coarse_blocks)
            def _():
                for d in range(1, T):
                    target = z - d if before else z + d

                    @pl.when((target >= 0) & (target < T))
                    def _():
                        spot = rows_recv.at[1 + z]
                        send(mine, mine, sent.at[3], spot, me, target).start()

    urgent = range(min(2, len(row_sets)))
    later_sets = range(len(urgent), len(row_sets))
    early = (z == owner(0)) | (z == owner(urgent[-1]))

    cut = leaf * LEAD // 8
    outward = jnp.where(parity == 0, left, right)
    leads = jnp.where((me < 2) & (z == 0), parity == 0, outward < lax.rem(me + 2 * step + R, R))

    def send_edge(source, first, high, begin=0, end=leaf):
        at = first + (count - 1 if high else 0)
        span = pl.ds(begin, end - begin)
        landing = beyond_leaf.at[0 if high else 1, span]
        target = right if high else left
        send(source.at[at, span], landing, sent.at[0], edge_recv.at[0], target, z).start()

    rounds = [0, 2, 3]

    def tell(k):
        for other in (left, right):
            pl.semaphore_signal(
                hello.at[rounds[k]], inc=1, device_id=(other, z), device_id_type=MESH
            )

    def hear(k):
        pl.semaphore_wait(hello.at[rounds[k]], 2)

    def pass_on(k):
        if compact:
            hear(k)
            tell(k + 1)

    def enter():
        if compact:
            pl.semaphore_wait(barrier, z + 2)
            tell(0)
        else:
            before = me - jnp.where(me > 0, 1, 0) - jnp.where(me == R - 1, 1, 0)
            pl.semaphore_wait(barrier, z + 2 + before)
            for k in range(2, R - 1):
                other = lax.rem(me + k, R)

                @pl.when(other < me)
                def _():
                    pl.semaphore_signal(
                        hello.at[0], inc=1, device_id=(other, z), device_id_type=MESH
                    )

        for k in range(1, T):

            @pl.when(z >= k)
            def _():
                pl.semaphore_signal(hello.at[1], inc=1, device_id=(me, z - k), device_id_type=MESH)

        for high in (0, 1):

            @pl.when(parity != high)
            def _():
                send_edge(x_hbm, 0, high)

            @pl.when(leads & (parity == high))
            def _():
                send_edge(x_hbm, 0, high, 0, cut)


    def coarse_rows():
        whole(coarse_in, load_sem.at[1]).wait()
        for r in range(block):
            wc[z * block + r] = jnp.concatenate([coarse_in[r, k] for k in range(4)], axis=1)
        send_rows(range(len(row_sets)), True)
        send_tables(True)

    def hear_planes():
        @pl.when(z < T - 1)
        def _():
            pl.semaphore_wait(hello.at[1], T - 1 - z)

    def early_rows():
        @pl.when(early)
        def _():
            hear_planes()
            send_rows(urgent, False)

    near_loads = [
        pltpu.make_async_copy(near_hbm.at[pl.ds(a, b - a)], nears[c], load_sem.at[5 + c])
        for c, (a, b) in enumerate(spans)
    ]
    edge_loads = [
        pltpu.make_async_copy(near_hbm.at[pl.ds(t, 1)], near_edges.at[pl.ds(k, 1)], load_sem.at[0])
        for k, t in enumerate((0, count - 1))
    ]
    load_sf = pltpu.make_async_copy(sf_hbm, sf, load_sem.at[2])
    load_tb = pltpu.make_async_copy(tb_hbm, tb, load_sem.at[1])

    def leaf_moment(t):
        cw0[2 + t] = dot(sb[t], xw[1 + t]).astype(BF16)

    def moments():
        load_sb.wait()
        whole(xw.at[pl.ds(0, 2)], load_sem.at[0]).wait()
        leaf_moment(0)
        leaf_moment(count - 1)
        for c, (a, b) in enumerate(spans):
            x_loads[c].wait()
            near_loads[c].start()
            for t in range(a, b):
                leaf_moment(t)
        for copy in edge_loads + [load_sf]:
            copy.start()

    def pair_matrix(level, j):
        first = firsts[level] + 2 * j
        return ef[first : first + 2].reshape(2 * rank, rank)

    def halo(level):
        ref, size = windows[level], sizes[level]
        if level == 0:
            both(lifts.at[0], lifts.at[3], lifts.at[1], lifts.at[2], 0)
        width, at = (2, 2) if level == 0 else (1, 3)
        both(
            ref.at[pl.ds(at, width)],
            ref.at[pl.ds(size + at, width)],
            ref.at[pl.ds(size, width)],
            ref.at[pl.ds(0, width)],
            level,
        )

    def upward(sending):
        load_ef.wait()
        low_pack = [pair_matrix(level, 0) for level in range(3)]
        high_pack = [pair_matrix(level, sizes[level + 1] - 1) for level in range(3)]
        lifts[0] = jnp.concatenate(low_pack + low_pack[:1], axis=1)
        lifts[1] = jnp.concatenate(high_pack + high_pack[:1], axis=1)
        for level in range(3):
            below, above = windows[level], windows[level + 1]
            for j in range(sizes[level + 1]):
                pair = below[2 + 2 * j : 4 + 2 * j].reshape(2 * rank, -1)
                above[2 + j] = dot_t(pair_matrix(level, j), pair).astype(BF16)
            if level == 0 and sending:
                halo(0)

    first_chip = (me < 2) & (z == 0)

    @pl.when(first_chip)
    def _():
        moments()
        upward(False)
        enter()
        halo(0)

    @pl.when(jnp.logical_not(first_chip))
    def _():
        enter()
        coarse_rows()
        moments()
        early_rows()
        pass_on(0)
        upward(True)

    for level in (1, 2, 3):
        halo(level)

    @pl.when(first_chip)
    def _():
        coarse_rows()
        early_rows()

    load_tb.start()
    for copy in load_lists:
        copy.wait()
    total = count * R

    def near_block(t, near, at, wanted):
        target = lax.rem(me * count + t + wanted + total, total)
        slot = jnp.where(
            near_list[0, t] == target, 0, jnp.where(near_list[1, t] == target, 1, 2)
        )
        return near[at, slot]

    def near_terms(t, near, at, first, last):
        blocks = [near_block(t, near, at, wanted) for wanted in range(first, last + 1)]
        points = xw[1 + t + first : 2 + t + last].reshape(-1, xw.shape[2])
        return dot(jnp.concatenate(blocks, axis=1), points)

    def near_span(c):
        near_loads[c].wait()
        for t in range(*spans[c]):
            part[t] = near_terms(t, nears[c], t - spans[c][0], -1, 1).astype(BF16)


    for c in range(len(spans)):
        near_span(c)
        if c == 0:

            @pl.when(jnp.logical_not(first_chip))
            def _():
                pass_on(1)

        if c < 2:

            @pl.when(first_chip)
            def _():
                pass_on(c)


    def transfer(row):
        return wc[row][:, 3 * rank :]

    def coarse_moment(cluster, at):
        lower, upper = transfer(2 * R + 2 * cluster), transfer(2 * R + 2 * cluster + 1)
        cr[cluster] = (dot_t(lower, cw3[at]) + dot_t(upper, cw3[at + 1])).astype(BF16)

    def gather_copy(source, target, k):
        spot = cr.at[pl.ds(source, 1)]
        return send(spot, spot, sent.at[gather_sent], gather_recv.at[k], target, z)

    @pl.when(jnp.logical_not(early))
    def _():
        hear_planes()

    send_rows(later_sets, False)
    send_tables(False)
    far_lists = [load(far_fine_hbm, far_fine, 5), load(far_coarse_hbm, far_coarse, 6)]

    if compact:
        hear(2)
    else:
        later = R - 1 - me - jnp.where(me == 0, 2, jnp.where(me == R - 1, 0, 1))

        @pl.when(later > 0)
        def _():
            pl.semaphore_wait(hello.at[0], later)

    receive_rows(range(1))
    coarse_moment(me, 2)

    def ring(offset):
        return lax.rem(me + offset + 2 * R, R)

    if compact:
        targets = [(ring(2 * step), 0), (ring(R // 2), 1), (ring(R // 2 + step), 1)]
    else:
        targets = [(ring(2 * k), me) for k in range(1, R // 2)] + [(twin, me)]
    for target, k in targets:
        gather_copy(me, target, k).start()

    for high in (0, 1):

        @pl.when(leads & (parity == high))
        def _():
            send_edge(xw, 1, high, cut, leaf)

    for high in (0, 1):

        @pl.when(jnp.logical_not(leads | first_chip) & (parity == high))
        def _():
            send_edge(xw, 1, high, 0, TRAIL * leaf // 8)

    whole(near_edges, load_sem.at[0]).wait()
    part[0] = near_terms(0, near_edges, 0, 0, 1).astype(BF16)
    part[count - 1] = near_terms(count - 1, near_edges, 1, -1, 0).astype(BF16)
    edge_block[0] = near_block(0, near_edges, 0, -1)
    edge_block[1] = near_block(count - 1, near_edges, 1, 1)

    load_sf.wait()
    for j in range(wf.shape[0]):
        wf[j] = jnp.concatenate([sf[j, 0], sf[j, 1], sf[j, 2], ef[j]], axis=1)

    for j in range(sizes[2]):
        both_rows = dot(pair_matrix(1, j), ef[firsts[2] + j]).astype(BF16)
        q1[2 * j : 2 * j + 2] = both_rows.reshape(2, rank, rank)
    for j in range(sizes[1]):
        both_rows = dot(pair_matrix(0, j), q1[j]).astype(BF16)
        q0[2 * j : 2 * j + 2] = both_rows.reshape(2, rank, rank)
    across = lax.broadcasted_iota(jnp.int32, (rank, rank), 0)
    down = lax.broadcasted_iota(jnp.int32, (rank, rank), 1)
    unit = jnp.where(across == down, 1.0, 0.0).astype(BF16)
    load_tb.wait()
    for t in range(count):
        tt[t] = dot_t(tb[t], jnp.concatenate([unit, q0[t]], axis=1)).astype(BF16)

    for high in (0, 1):

        @pl.when(jnp.logical_not(leads | first_chip) & (parity == high))
        def _():
            send_edge(xw, 1, high, TRAIL * leaf // 8, leaf)

    whole(cw0.at[pl.ds(0, 5)], halo_recv.at[0]).wait()
    for level in range(3):
        below, above = windows[level], windows[level + 1]
        size = sizes[level]
        if level == 0:
            whole(cw0.at[pl.ds(0, 6)], halo_recv.at[1]).wait()
        from_left = lifts[2][:, level * rank : (level + 1) * rank]
        from_right = lifts[3][:, level * rank : (level + 1) * rank]
        low_pair = below[0:2].reshape(2 * rank, -1)
        high_pair = below[size + 2 : size + 4].reshape(2 * rank, -1)
        above[1] = dot_t(from_left, low_pair).astype(BF16)
        above[size // 2 + 2] = dot_t(from_right, high_pair).astype(BF16)

    for high in (0, 1):

        @pl.when(jnp.logical_not(leads) & first_chip & (parity == high))
        def _():
            send_edge(xw, 1, high)

    if compact:

        receive_rows(range(1, 2))
        coarse_moment(near_by, 4 * parity)
        gather_copy(near_by, twin, 1).start()

    for copy in far_lists:
        copy.wait()

    for i in range(2):
        row = 2 * R + 2 * me + i
        parts = [
            cw3[jnp.minimum(lax.rem(far_coarse[s, row] - 2 * me + 2 + 2 * R, 2 * R), 5)]
            for s in range(3)
        ]
        f3[i] = dot(wc[row][:, : 3 * rank], jnp.concatenate(parts, axis=0)).astype(BF16)
    upper = f3
    for level, below in ((2, f2), (1, f1), (0, f0)):
        m = sizes[level]
        n = m * R
        for i in range(m):
            row = firsts[level] + i
            parts = [
                windows[level][jnp.minimum(lax.rem(far_fine[s, row] - m * me + 2 + n, n), m + 3)]
                for s in range(3)
            ] + [upper[i // 2]]
            below[i] = dot(wf[row], jnp.concatenate(parts, axis=0)).astype(BF16)
        upper = below

    receive_rows(later_sets)
    if not compact:
        for k in range(1, T):
            other = lax.rem(z + k, T)
            theirs = wc.at[pl.ds(other * block, block)]

            @pl.when(other < coarse_blocks)
            def _():
                spot = rows_recv.at[1 + other]
                send(theirs, theirs, sent.at[3], spot, me, other).wait_recv()

    def upper_rows():
        return jnp.concatenate([transfer(2 * R + 2 * me + i) for i in range(2)], axis=0)

    if compact:
        down = dot(upper_rows(), wc[R + me]).astype(BF16)
        across = wc[4 + me // 2][:, :rank]
        lifted = [dot_n(across, transfer(R + 2 * opposite + i)).astype(BF16) for i in range(2)]
        far_up = dot(down[:, 3 * rank :], jnp.concatenate(lifted, axis=1)).astype(BF16)
        coarse_matrix = jnp.concatenate([down[:, : 3 * rank], far_up], axis=1)

    if compact:
        beyond = ring(-2 * step)
        gather_copy(beyond, me, 0).wait_recv()
        gather_copy(beyond, twin, 1).start()
        whole(cr.at[pl.ds(0, 4)], gather_recv.at[1]).wait()
        passes = 5
    else:
        for k in range(1, R // 2):
            gather_copy(ring(2 * k), me, ring(2 * k)).wait_recv()
            gather_copy(ring(2 * k), twin, ring(2 * k)).start()
        for k in range(R // 2):
            other = lax.rem(twin + 2 * k, R)
            gather_copy(other, me, other).wait_recv()
        passes = R - 1
    def coarse(n, index):
        return cr[index] if n == R else cu[n - 4 + index]

    def lift(n, j):
        lifted = dot_t(transfer(2 * n + 2 * j), coarse(2 * n, 2 * j)) + dot_t(
            transfer(2 * n + 2 * j + 1), coarse(2 * n, 2 * j + 1)
        )
        return lifted.astype(BF16)

    if compact:
        parts = [cr[far_coarse[s, R + me]] for s in range(3)]
        parts += [cr[2 * opposite], cr[2 * opposite + 1]]
        pair = dot(coarse_matrix, jnp.concatenate(parts, axis=0))
    else:
        n = R // 2
        while n >= 4:
            for j in range(n):
                cu[n - 4 + j] = lift(n, j)
            n //= 2
        n = 4
        value = None
        while n <= R:
            row = n + me // (R // n)
            if n == 4:
                value = dot(wc[row][:, :rank], coarse(n, far_coarse[0, row]))
            else:
                parts = [coarse(n, far_coarse[s, row]) for s in range(3)] + [value]
                value = dot(wc[row], jnp.concatenate(parts, axis=0))
            value = value.astype(BF16)
            n *= 2
        pair = dot(upper_rows(), value)
    top[...] = pair.astype(BF16).reshape(top.shape)

    whole(xw.at[pl.ds(0, 2)], edge_recv.at[0]).wait()
    for k in range(len(row_sets)):

        @pl.when(z == owner(k))
        def _():
            whole(wc.at[pl.ds(0, row_sets[k][1] * (T - 1))], sent.at[rows_sent + k]).wait()

    if not compact:

        @pl.when(z < coarse_blocks)
        def _():
            whole(wc.at[pl.ds(0, block * (T - 1))], sent.at[3]).wait()

    if compact:
        leaves, over = divmod(2 * leaf + (11 + passes) * rank, leaf)
        assert over == 0
        whole(xw.at[pl.ds(0, leaves)], sent.at[0]).wait()
    else:
        whole(xw.at[pl.ds(0, 2)], sent.at[0]).wait()
        whole(cw0.at[pl.ds(0, 11)], sent.at[halo_sent]).wait()
        whole(cr.at[pl.ds(0, passes)], sent.at[gather_sent]).wait()


def finish(part, tt, f, top, edge_block, beyond_leaf, out_hbm, out, sem):
    count = part.shape[0]
    middle = count // 2
    order = [*range(1, middle), 0, count - 1, *range(middle, count - 1)]
    for t in order:
        matrix, rows = tt[t], jnp.concatenate([f[t], top[t * top.shape[0] // count]], axis=0)
        if t in (0, count - 1):
            matrix = jnp.concatenate([edge_block[t // (count - 1)], matrix], axis=1)
            rows = jnp.concatenate([beyond_leaf[t // (count - 1)], rows], axis=0)
        parts = 4 if t == order[0] else 1
        size = part.shape[1] // parts
        for k in range(parts):
            span = slice(k * size, (k + 1) * size)
            total = part[t, span].astype(F32) + dot(matrix[span], rows)
            out[t, span] = total.astype(BF16)
            spot = pl.ds(k * size, size)
            pltpu.make_async_copy(out.at[t, spot], out_hbm.at[t, spot], sem).start()
    pltpu.make_async_copy(out, out_hbm, sem).wait()


def body(
    sources,
    near_blocks,
    near_list,
    source_basis,
    target_basis,
    transfer_fine,
    transfer_coarse,
    couple_fine,
    couple_coarse,
    far_fine,
    far_coarse,
):
    count, _, leaf, _ = near_blocks.shape
    rank = source_basis.shape[2]
    width = sources.shape[1]
    R, T = lax.axis_size("rows"), lax.axis_size("rhs")
    fine = transfer_fine.shape[0]
    block = transfer_coarse.shape[0]
    cuts = [1, 1 + (count - 2) // 4, count // 2, count - 1 - (count - 2) // 4, count - 1]
    spans = list(zip(cuts[:-1], cuts[1:]))
    dims = (count, leaf, rank, R, T, spans)
    hbm = pl.BlockSpec(memory_space=pltpu.HBM)
    vmem = pl.BlockSpec(memory_space=pltpu.VMEM)

    def in_hbm(a):
        return pltpu.with_memory_space_constraint(a, pltpu.HBM)

    def moments(clusters):
        return pltpu.VMEM((clusters, rank, width), BF16)

    dma = pltpu.SemaphoreType.DMA
    target = in_hbm(jnp.swapaxes(target_basis, 1, 2))
    results = pl.pallas_call(
        lambda *refs: kernel(dims, *refs),
        name="tree_apply",
        out_shape=[
            pltpu.VMEM((count, leaf, width), BF16),
            pltpu.VMEM((count, leaf, 2 * rank), BF16),
            moments(count),
            moments(count // 8),
            pltpu.VMEM((2, leaf, leaf), BF16),
            pltpu.VMEM((2, leaf, width), BF16),
        ],
        in_specs=[hbm] * 11,
        out_specs=[vmem] * 6,
        scratch_shapes=[
            pltpu.SMEM(near_list.shape[::-1], jnp.int32),
            pltpu.SMEM(far_fine.shape[::-1], jnp.int32),
            pltpu.SMEM(far_coarse.shape[::-1], jnp.int32),
            pltpu.VMEM((count + 2, leaf, width), BF16),
            [pltpu.VMEM((b - a,) + near_blocks.shape[1:], BF16) for a, b in spans],
            pltpu.VMEM((2,) + near_blocks.shape[1:], BF16),
            pltpu.VMEM((count, rank, leaf), BF16),
            pltpu.VMEM((count, rank, leaf), BF16),
            pltpu.VMEM(transfer_fine.shape, BF16),
            pltpu.VMEM(couple_fine.shape, BF16),
            pltpu.VMEM((block, 4, rank, rank), BF16),
            pltpu.VMEM((fine, rank, 4 * rank), BF16),
            pltpu.VMEM((block * T, rank, 4 * rank), BF16),
            moments(count + 4),
            moments(count // 2 + 4),
            moments(count // 4 + 4),
            moments(count // 8 + 4),
            moments(R),
            moments(R),
            moments(count // 8),
            moments(count // 4),
            moments(count // 2),
            pltpu.VMEM((4, 2 * rank, 4 * rank), BF16),
            pltpu.VMEM((count // 2, rank, rank), BF16),
            pltpu.VMEM((count, rank, rank), BF16),
            dma((5 + len(spans),)),
            dma((6 if R == 8 else 5,)),
            dma((1,)),
            dma((2,)),
            dma((2 if R == 8 else R,)),
            dma((5 if R == 8 else 1 + T,)),
            pltpu.SemaphoreType.REGULAR((4 if R == 8 else 2,)),
        ],
        compiler_params=pltpu.CompilerParams(
            collective_id=0, has_side_effects=True, vmem_limit_bytes=40 * MIB
        ),
    )(
        in_hbm(sources.reshape(count, leaf, width)),
        in_hbm(near_blocks),
        in_hbm(near_list.T),
        in_hbm(jnp.swapaxes(source_basis, 1, 2)),
        target,
        in_hbm(transfer_fine),
        in_hbm(transfer_coarse),
        in_hbm(couple_fine),
        in_hbm(couple_coarse),
        in_hbm(far_fine.T),
        in_hbm(far_coarse.T),
    )
    out = pl.pallas_call(
        finish,
        name="far_add",
        out_shape=jax.ShapeDtypeStruct((count, leaf, width), BF16),
        in_specs=[vmem] * 6,
        out_specs=pl.BlockSpec(memory_space=pl.ANY),
        scratch_shapes=[pltpu.VMEM((count, leaf, width), BF16), dma],
        compiler_params=pltpu.CompilerParams(vmem_limit_bytes=20 * MIB),
    )(*results)
    return out.reshape(count * leaf, width)


def solution(mesh):
    in_specs = (
        P("rows", "rhs"),
        P("rows", None, None, None),
        P("rows", None),
        P("rows", None, None),
        P("rows", None, None),
        P("rows", None, None),
        P("rhs", None, None),
        P("rows", None, None, None),
        P("rhs", None, None, None),
        P("rows", None),
        P(),
    )
    out_specs = P("rows", "rhs")
    return jax.shard_map(body, mesh=mesh, in_specs=in_specs, out_specs=out_specs, check_vma=False)
```
